32 devices in a mesh: dp: 1 (over z), tp: 32 (over y, x, core).
Axes of the slice: x: 4, y: 4, z: 1, core: 2. Of those that a mesh axis runs over, the one named last changes fastest.
The devices are a block of a 4x4x8 slice.
Arguments:
- hidden: bfloat16 [8192, 1024], P(('dp', 'tp'))
- norm_gain: float32 [1024], replicated
- w_query: bfloat16 [1024, 128, 128], P(None, 'tp')
- w_key: bfloat16 [1024, 128, 128], P(None, 'tp')
- w_value: bfloat16 [1024, 128, 128], P(None, 'tp')
Outputs:
- output 1: bfloat16 [8192, 128, 128], P('dp', 'tp')
- output 2: bfloat16 [8192, 128, 128], P('dp', 'tp')
- output 3: bfloat16 [8192, 128, 128], P('dp', 'tp')
All inputs are finite; a program needn't handle non-finite values.
Results may differ from the reference program's by a relative error of at most 0.001.
Values are sent between devices in bfloat16 or wider.
A program may use at most 768 MiB of HBM per device.

```python
import jax
import jax.numpy as jnp
from jax import lax

TOKENS = 8192
MODEL_DIM = 1024
Q_HEADS = 128
KV_COUNT = 128
HEAD_DIM = 128


def setup_inputs(seed: int = 0, part: int = 0) -> dict:
    base_key = jax.random.key(seed)
    part_key = jax.random.fold_in(base_key, part)
    shared = jax.random.split(base_key, 4)
    fan_scale = MODEL_DIM ** -0.5
    hidden = jax.random.normal(part_key, (TOKENS, MODEL_DIM), jnp.float32).astype(jnp.bfloat16)
    norm_gain = jax.random.uniform(shared[0], (MODEL_DIM,), jnp.float32, 0.5, 1.5)
    w_query = (jax.random.normal(shared[1], (MODEL_DIM, Q_HEADS, HEAD_DIM), jnp.float32) * fan_scale).astype(jnp.bfloat16)
    w_key = (jax.random.normal(shared[2], (MODEL_DIM, KV_COUNT, HEAD_DIM), jnp.float32) * fan_scale).astype(jnp.bfloat16)
    w_value = (jax.random.normal(shared[3], (MODEL_DIM, KV_COUNT, HEAD_DIM), jnp.float32) * fan_scale).astype(jnp.bfloat16)
    return {"hidden": hidden, "norm_gain": norm_gain, "w_query": w_query, "w_key": w_key, "w_value": w_value}


def reference(hidden, norm_gain, w_query, w_key, w_value):
    hidden_f32 = hidden.astype(jnp.float32)
    mean_sq = jnp.mean(hidden_f32 * hidden_f32, axis=-1, keepdims=True)
    normed = (hidden_f32 * lax.rsqrt(mean_sq + 1e-6) * norm_gain).astype(jnp.bfloat16)

    def project(weight):
        head_count = weight.shape[1]
        flat_out = jnp.dot(normed, weight.reshape(MODEL_DIM, head_count * HEAD_DIM), preferred_element_type=jnp.float32)
        return flat_out.astype(jnp.bfloat16).reshape(TOKENS, head_count, HEAD_DIM)

    return (project(w_query), project(w_key), project(w_value))
```

```python
import functools
import math

import jax
import jax.numpy as jnp
from jax import lax
from jax.experimental import pallas as pl
from jax.experimental.pallas import tpu as pltpu
from jax.sharding import PartitionSpec as P

MESH = pl.DeviceIdType.MESH
CORES = 2
LANES = 128

ORDER = ((0, 0), (-1, 0), (1, 0), (0, -1), (0, 1), (2, 0), (-1, -1), (-1, 1), (1, -1), (1, 1), (2, -1), (2, 1), (0, 2), (-1, 2), (1, 2), (2, 2))
XP, XM, YP, YM = range(4)


def gather_project(side, x_hbm, g_ref, wq_hbm, wk_hbm, wv_hbm, q_ref, k_ref, v_ref, xbuf, tokens, wraw, wflat, stage,
                   in_sem, send_sem, pair_send_sem, link_sem, pair_sem):
    rows, depth = xbuf.shape
    half, quarter = rows // 2, rows // 4
    heads = wraw.shape[1] // depth
    cols = heads * LANES
    me = lax.axis_index("tp")
    core = lax.rem(me, CORES)
    chip = me // CORES
    my_x, my_y = lax.rem(chip, side), chip // side

    def chip_at(dx, dy):
        return lax.rem(my_y + dy + side, side) * side + lax.rem(my_x + dx + side, side)

    def device(chip_index, core_index):
        return {"tp": chip_index * CORES + core_index}

    neighbour = (chip_at(1, 0), chip_at(-1, 0), chip_at(0, 1), chip_at(0, -1))
    other = 1 - core

    copies_in = [pltpu.make_async_copy(x_hbm, xbuf, in_sem.at[0])]
    for i, w in enumerate((wq_hbm, wk_hbm, wv_hbm)):
        copies_in.append(pltpu.make_async_copy(w, wraw.at[i], in_sem.at[1 + i]))
    for copy in copies_in:
        copy.start()

    barrier = pltpu.get_barrier_semaphore()
    for chip_index in neighbour:
        pl.semaphore_signal(barrier, inc=1, device_id=device(chip_index, core), device_id_type=MESH)
    pl.semaphore_signal(barrier, inc=1, device_id=device(chip, other), device_id_type=MESH)

    def piece(dx, dy, is_q, part=None):
        start = chip_at(dx, dy) * (CORES * rows) + is_q * (CORES * half) + core * half
        if part is None:
            return tokens.at[pl.ds(pl.multiple_of(start, half), half)]
        return tokens.at[pl.ds(pl.multiple_of(start + part * quarter, quarter), quarter)]

    def link_copy(link, seq, ref):
        return pltpu.make_async_remote_copy(
            src_ref=ref, dst_ref=ref, send_sem=send_sem.at[link], recv_sem=link_sem.at[link, seq],
            device_id=device(neighbour[link], core), device_id_type=MESH)

    def pair_copy(step, is_q):
        dx, dy = ORDER[step]
        ref = piece(dy, dx, 1) if is_q else piece(dx, dy, 0)
        return pltpu.make_async_remote_copy(
            src_ref=ref, dst_ref=ref, send_sem=pair_send_sem.at[step % 4], recv_sem=pair_sem.at[step, is_q],
            device_id=device(chip, other), device_id_type=MESH)

    def send(link, seq):
        is_y = link >= YP
        back = -1 if link in (XP, YP) else 1
        part = 0 if link in (XP, YP) else 1
        lateral = {1: 0, 3: -1, 4: 1, 5: 2, 6: 0, 7: -1, 8: 1, 9: 2}
        if seq == 0:
            off, second, sub = (0, 0), 0, None
        elif seq == 2:
            off, second, sub = (back, 0), 0, part
        elif seq in (1, 3, 4, 5):
            off, second, sub = (0, lateral[seq]), 1, None
        else:
            off, second, sub = (back, lateral[seq]), 1, part
        if is_y:
            off = (off[1], off[0])
        link_copy(link, seq, piece(*off, second ^ int(is_y), sub)).start()

    def arrived(link, seq):
        n = quarter if seq in (2, 6, 7, 8, 9) else half
        link_copy(link, seq, tokens.at[pl.ds(0, n)]).wait_recv()

    links = (XP, XM, YP, YM)

    copies_in[0].wait()
    own = chip * (CORES * rows) + core * half
    norm_rows = 16

    def normalize(i, _):
        xf = xbuf[pl.ds(pl.multiple_of(i * norm_rows, norm_rows), norm_rows), :].astype(jnp.float32)
        mean_sq = jnp.mean(xf * xf, axis=-1, keepdims=True)
        n = (xf * lax.rsqrt(mean_sq + 1e-6) * g_ref[...]).astype(jnp.bfloat16)
        per_half = half // norm_rows
        dst = own + (i // per_half) * (CORES * half) + lax.rem(i, per_half) * norm_rows
        tokens[pl.ds(pl.multiple_of(dst, norm_rows), norm_rows), :] = n
        return 0

    lax.fori_loop(0, rows // norm_rows, normalize, 0)

    pl.semaphore_wait(barrier, 5)
    for seq in (0, 1):
        for link in links:
            send(link, seq)
        if seq == 0:
            pair_copy(0, 0).start()
            pair_copy(0, 1).start()

    wrows = stage.shape[1] // heads
    for i in range(3):
        copies_in[1 + i].wait()

        def relayout(j, _, i=i):
            src = pl.multiple_of(j * (wrows * heads), wrows * heads)
            dst = pl.multiple_of(j * wrows, wrows)
            stage[i] = wraw[i, pl.ds(src, wrows * heads), :].astype(jnp.float32)
            for h in range(heads):
                wflat[pl.ds(dst, wrows), pl.ds(i * cols + h * LANES, LANES)] = stage[i, pl.ds(h, wrows, stride=heads), :].astype(jnp.bfloat16)
            return 0

        lax.fori_loop(0, depth // wrows, relayout, 0)

    events = {
        1: ([(l, 0) for l in links], [(l, s) for s in (2, 3, 4) for l in links], (1, 2)),
        3: ([(l, 1) for l in links], [], (3, 4)),
        5: ([(l, 2) for l in links], [(l, s) for s in (5, 6) for l in links], (5,)),
        6: ([(l, 3) for l in links], [(l, 7) for l in links], (6, 7)),
        8: ([(l, 4) for l in links], [(l, 8) for l in links], (8, 9)),
        10: ([(l, 5) for l in links], [(l, 9) for l in links], (10, 11)),
        12: ([(l, 6) for l in links], [], (12,)),
        13: ([(l, 7) for l in links], [], (13,)),
        14: ([(l, 8) for l in links], [], (14,)),
        15: ([(l, 9) for l in links], [], (15,)),
    }

    def body(s, _):
        step, sub = s // 2, lax.rem(s, 2)
        for at, (waits, sends, pairs) in events.items():
            @pl.when(s == 2 * at)
            def _(waits=waits, sends=sends, pairs=pairs):
                for w in waits:
                    arrived(*w)
                for x in sends:
                    send(*x)
                for p in pairs:
                    pair_copy(p, 0).start()
                    pair_copy(p, 1).start()

        @pl.when(sub == 1)
        def _():
            for is_q in range(2):
                pltpu.make_async_remote_copy(
                    src_ref=tokens.at[pl.ds(0, half)], dst_ref=tokens.at[pl.ds(0, half)], send_sem=pair_send_sem.at[0],
                    recv_sem=pair_sem.at[step, is_q], device_id=device(chip, other), device_id_type=MESH).wait_recv()

        dx, dy = jnp.int32(0), jnp.int32(0)
        for k, (ox, oy) in enumerate(ORDER):
            dx = jnp.where(step == k, ox, dx)
            dy = jnp.where(step == k, oy, dy)
        plane = core + sub * (1 - 2 * core)
        chips = (chip_at(dx, dy), chip_at(dy, dx))
        src = [pl.multiple_of(chips[i] * (CORES * rows) + i * (CORES * half) + plane * half, half) for i in range(2)]
        dst = [pl.multiple_of(((chips[i] * CORES + plane) * rows + i * half) * heads, half * heads) for i in range(2)]
        lhs = jnp.concatenate([tokens[pl.ds(src[i], half), :] for i in range(2)], axis=0)
        for i, out in enumerate((q_ref, k_ref, v_ref)):
            for b in range(cols // 256):
                acc = jnp.dot(lhs, wflat[:, pl.ds(i * cols + b * 256, 256)], preferred_element_type=jnp.float32)
                for h in range(2):
                    stage[i, pl.ds(b * 2 + h, rows, stride=heads), :] = acc[:, h * LANES:(h + 1) * LANES]
            for j in range(2):
                out[pl.ds(dst[j], half * heads), :] = stage[i, pl.ds(j * half * heads, half * heads), :].astype(jnp.bfloat16)
        return 0

    lax.fori_loop(0, 2 * len(ORDER), body, 0)

    per_link = 5 * half + 5 * quarter
    for link in links:
        link_copy(link, 0, tokens.at[pl.ds(0, per_link)]).wait_send()
    for i in range(4):
        ref = tokens.at[pl.ds(0, 8 * half)]
        pltpu.make_async_remote_copy(
            src_ref=ref, dst_ref=ref, send_sem=pair_send_sem.at[i], recv_sem=pair_sem.at[0, 0],
            device_id=device(chip, other), device_id_type=MESH).wait_send()


def drain(pieces, *refs):
    ins, outs, sem = refs[:3], refs[3:6], refs[6]
    n = ins[0].shape[0] // pieces
    copies = [pltpu.make_async_copy(ins[i].at[pl.ds(p * n, n)], outs[i].at[pl.ds(p * n, n)], sem.at[i, p])
              for p in range(pieces) for i in range(3)]
    for copy in copies:
        copy.start()
    for copy in copies:
        copy.wait()


def solution(mesh):
    size = mesh.shape["tp"]
    side = math.isqrt(size // CORES)
    assert side * side * CORES == size and side * side == len(ORDER)

    def local_step(x, gain, wq, wk, wv):
        rows, depth = x.shape
        heads = wq.shape[1]
        total = rows * size
        flat = [w.reshape(depth * heads, LANES) for w in (wq, wk, wv)]
        vmem_out = pltpu.VMEM((total * heads, LANES), jnp.bfloat16)
        outs = pl.pallas_call(
            functools.partial(gather_project, side),
            out_shape=(vmem_out,) * 3,
            in_specs=[pl.BlockSpec(memory_space=pl.ANY), pl.BlockSpec(memory_space=pltpu.VMEM)] + [pl.BlockSpec(memory_space=pl.ANY)] * 3,
            out_specs=[pl.BlockSpec(memory_space=pltpu.VMEM)] * 3,
            scratch_shapes=[
                pltpu.VMEM((rows, depth), jnp.bfloat16),
                pltpu.VMEM((total, depth), jnp.bfloat16),
                pltpu.VMEM((3, depth * heads, LANES), jnp.bfloat16),
                pltpu.VMEM((depth, 3 * heads * LANES), jnp.bfloat16),
                pltpu.VMEM((3, rows * heads, LANES), jnp.float32),
                pltpu.SemaphoreType.DMA((4,)),
                pltpu.SemaphoreType.DMA((4,)),
                pltpu.SemaphoreType.DMA((4,)),
                pltpu.SemaphoreType.DMA((4, 10)),
                pltpu.SemaphoreType.DMA((len(ORDER), 2)),
            ],
            compiler_params=pltpu.CompilerParams(collective_id=0, has_side_effects=True, vmem_limit_bytes=36 * 1024 * 1024),
            name="gather_project",
        )(x, gain.reshape(1, depth), *flat)
        out = jax.ShapeDtypeStruct((total * heads, LANES), jnp.bfloat16)
        outs = pl.pallas_call(
            functools.partial(drain, 4),
            out_shape=(out,) * 3,
            in_specs=[pl.BlockSpec(memory_space=pltpu.VMEM)] * 3,
            out_specs=[pl.BlockSpec(memory_space=pl.ANY)] * 3,
            scratch_shapes=[pltpu.SemaphoreType.DMA((3, 4))],
            compiler_params=pltpu.CompilerParams(vmem_limit_bytes=1024 * 1024),
            name="drain",
        )(*outs)
        return tuple(o.reshape(total, heads, LANES) for o in outs)

    row_spec = P(("dp", "tp"), None)
    head_spec = P(None, "tp", None)
    out_spec = P("dp", "tp", None)
    return jax.shard_map(local_step, mesh=mesh, in_specs=(row_spec, P(None), head_spec, head_spec, head_spec),
                         out_specs=(out_spec, out_spec, out_spec), check_vma=False)
```

```python
import functools
import math

import jax
import jax.numpy as jnp
from jax import lax
from jax.experimental import pallas as pl
from jax.experimental.pallas import tpu as pltpu
from jax.sharding import PartitionSpec as P

MESH = pl.DeviceIdType.MESH
CORES = 2
LANES = 128

ORDER = ((0, 0), (-1, 0), (1, 0), (0, -1), (0, 1), (2, 0), (-1, -1), (-1, 1), (1, -1), (1, 1), (2, -1), (2, 1), (0, 2), (-1, 2), (1, 2), (2, 2))
XP, XM, YP, YM = range(4)


TAIL = 2
VMEM_LIMIT = 63438848 - 28311552 - TAIL * 1048576


def places(side, rows, heads, chip_at, step, plane):
    half = rows // 2
    dx, dy = jnp.int32(0), jnp.int32(0)
    for k, (ox, oy) in enumerate(ORDER):
        dx = jnp.where(step == k, ox, dx)
        dy = jnp.where(step == k, oy, dy)
    chips = (chip_at(dx, dy), chip_at(dy, dx))
    src = [pl.multiple_of(chips[i] * (CORES * rows) + i * (CORES * half) + plane * half, half) for i in range(2)]
    dst = [pl.multiple_of(((chips[i] * CORES + plane) * rows + i * half) * heads, half * heads) for i in range(2)]
    return src, dst


def project(tokens, wflat, stage, src, half, outs):
    lhs = jnp.concatenate([tokens[pl.ds(r, half), :] for r in src], axis=0)
    heads = wflat.shape[1] // (3 * LANES)
    cols = heads * LANES
    for i, (out, dst) in enumerate(outs):
        for b in range(cols // 256):
            acc = jnp.dot(lhs, wflat[:, pl.ds(i * cols + b * 256, 256)], preferred_element_type=jnp.float32)
            for h in range(2):
                stage[i, pl.ds(b * 2 + h, 2 * half, stride=heads), :] = acc[:, h * LANES:(h + 1) * LANES]
        for j in range(2):
            out[pl.ds(dst[j], half * heads), :] = stage[i, pl.ds(j * half * heads, half * heads), :].astype(jnp.bfloat16)


def gather_project(side, x_hbm, g_ref, wq_hbm, wk_hbm, wv_hbm, q_ref, k_ref, v_ref, last, wflat, xbuf, tokens, wraw, stage,
                   in_sem, send_sem, pair_send_sem, link_sem, pair_sem):
    rows, depth = xbuf.shape
    half, quarter = rows // 2, rows // 4
    heads = wraw.shape[1] // depth
    cols = heads * LANES
    me = lax.axis_index("tp")
    core = lax.rem(me, CORES)
    chip = me // CORES
    my_x, my_y = lax.rem(chip, side), chip // side

    def chip_at(dx, dy):
        return lax.rem(my_y + dy + side, side) * side + lax.rem(my_x + dx + side, side)

    def device(chip_index, core_index):
        return {"tp": chip_index * CORES + core_index}

    neighbour = (chip_at(1, 0), chip_at(-1, 0), chip_at(0, 1), chip_at(0, -1))
    other = 1 - core

    copies_in = [pltpu.make_async_copy(x_hbm, xbuf, in_sem.at[0])]
    for i, w in enumerate((wq_hbm, wk_hbm, wv_hbm)):
        copies_in.append(pltpu.make_async_copy(w, wraw.at[i], in_sem.at[1 + i]))
    for copy in copies_in:
        copy.start()

    barrier = pltpu.get_barrier_semaphore()
    for chip_index in neighbour:
        pl.semaphore_signal(barrier, inc=1, device_id=device(chip_index, core), device_id_type=MESH)
    pl.semaphore_signal(barrier, inc=1, device_id=device(chip, other), device_id_type=MESH)

    def piece(dx, dy, is_q, part=None):
        start = chip_at(dx, dy) * (CORES * rows) + is_q * (CORES * half) + core * half
        if part is None:
            return tokens.at[pl.ds(pl.multiple_of(start, half), half)]
        return tokens.at[pl.ds(pl.multiple_of(start + part * quarter, quarter), quarter)]

    def last_piece(step, is_q, part=None):
        start = ((step - len(ORDER) + TAIL) * 2 + is_q) * (CORES * half) + core * half
        if part is None:
            return last.at[pl.ds(pl.multiple_of(start, half), half)]
        return last.at[pl.ds(pl.multiple_of(start + part * quarter, quarter), quarter)]

    def link_copy(link, seq, ref, dst=None):
        return pltpu.make_async_remote_copy(
            src_ref=ref, dst_ref=ref if dst is None else dst, send_sem=send_sem.at[link], recv_sem=link_sem.at[link, seq],
            device_id=device(neighbour[link], core), device_id_type=MESH)

    def pair_copy(step, is_q):
        dx, dy = ORDER[step]
        if step >= len(ORDER) - TAIL:
            ref = last_piece(step, is_q)
        else:
            ref = piece(dy, dx, 1) if is_q else piece(dx, dy, 0)
        return pltpu.make_async_remote_copy(
            src_ref=ref, dst_ref=ref, send_sem=pair_send_sem.at[step % 4], recv_sem=pair_sem.at[step, is_q],
            device_id=device(chip, other), device_id_type=MESH)

    def send(link, seq):
        is_y = link >= YP
        back = -1 if link in (XP, YP) else 1
        part = 0 if link in (XP, YP) else 1
        lateral = {1: 0, 3: -1, 4: 1, 5: 2, 6: 0, 7: -1, 8: 1, 9: 2}
        if seq == 0:
            off, second, sub = (0, 0), 0, None
        elif seq == 2:
            off, second, sub = (back, 0), 0, part
        elif seq in (1, 3, 4, 5):
            off, second, sub = (0, lateral[seq]), 1, None
        else:
            off, second, sub = (back, lateral[seq]), 1, part
        if is_y:
            off = (off[1], off[0])
        step = len(ORDER) - 10 + seq
        dst = last_piece(step, 1 - int(is_y), sub) if step >= len(ORDER) - TAIL else None
        link_copy(link, seq, piece(*off, second ^ int(is_y), sub), dst).start()

    def arrived(link, seq):
        n = quarter if seq in (2, 6, 7, 8, 9) else half
        link_copy(link, seq, tokens.at[pl.ds(0, n)]).wait_recv()

    links = (XP, XM, YP, YM)

    copies_in[0].wait()
    own = chip * (CORES * rows) + core * half
    norm_rows = 16

    def normalize(i, _):
        xf = xbuf[pl.ds(pl.multiple_of(i * norm_rows, norm_rows), norm_rows), :].astype(jnp.float32)
        mean_sq = jnp.mean(xf * xf, axis=-1, keepdims=True)
        n = (xf * lax.rsqrt(mean_sq + 1e-6) * g_ref[...]).astype(jnp.bfloat16)
        per_half = half // norm_rows
        dst = own + (i // per_half) * (CORES * half) + lax.rem(i, per_half) * norm_rows
        tokens[pl.ds(pl.multiple_of(dst, norm_rows), norm_rows), :] = n
        return 0

    lax.fori_loop(0, rows // norm_rows, normalize, 0)

    pl.semaphore_wait(barrier, 5)
    for seq in (0, 1):
        for link in links:
            send(link, seq)
        if seq == 0:
            pair_copy(0, 0).start()
            pair_copy(0, 1).start()

    wrows = stage.shape[1] // heads
    for i in range(3):
        copies_in[1 + i].wait()

        def relayout(j, _, i=i):
            src = pl.multiple_of(j * (wrows * heads), wrows * heads)
            dst = pl.multiple_of(j * wrows, wrows)
            stage[i] = wraw[i, pl.ds(src, wrows * heads), :].astype(jnp.float32)
            for h in range(heads):
                wflat[pl.ds(dst, wrows), pl.ds(i * cols + h * LANES, LANES)] = stage[i, pl.ds(h, wrows, stride=heads), :].astype(jnp.bfloat16)
            return 0

        lax.fori_loop(0, depth // wrows, relayout, 0)

    events = {
        1: ([(l, 0) for l in links], [(l, s) for s in (2, 3, 4) for l in links], (1, 2)),
        3: ([(l, 1) for l in links], [], (3, 4)),
        5: ([(l, 2) for l in links], [(l, s) for s in (5, 6) for l in links], (5,)),
        6: ([(l, 3) for l in links], [(l, 7) for l in links], (6, 7)),
        8: ([(l, 4) for l in links], [(l, 8) for l in links], (8, 9)),
        10: ([(l, 5) for l in links], [(l, 9) for l in links], (10, 11)),
        12: ([(l, 6) for l in links], [], (12,)),
        13: ([(l, 7) for l in links], [], (13,)),
        14: ([(l, 8) for l in links], [], (14,)),
        15: ([(l, 9) for l in links], [], (15,)),
    }

    def body(s, _):
        step, sub = s // 2, lax.rem(s, 2)
        for at, (waits, sends, pairs) in events.items():
            @pl.when(s == 2 * at)
            def _(waits=waits, sends=sends, pairs=pairs):
                for w in waits:
                    arrived(*w)
                for x in sends:
                    send(*x)
                for p in pairs:
                    pair_copy(p, 0).start()
                    pair_copy(p, 1).start()

        @pl.when(sub == 1)
        def _():
            for is_q in range(2):
                pltpu.make_async_remote_copy(
                    src_ref=tokens.at[pl.ds(0, half)], dst_ref=tokens.at[pl.ds(0, half)], send_sem=pair_send_sem.at[0],
                    recv_sem=pair_sem.at[step, is_q], device_id=device(chip, other), device_id_type=MESH).wait_recv()

        @pl.when(step < len(ORDER) - TAIL)
        def _():
            src, dst = places(side, rows, heads, chip_at, step, core + sub * (1 - 2 * core))
            project(tokens, wflat, stage, src, half, ((q_ref, dst), (k_ref, dst), (v_ref, dst)))
        return 0

    lax.fori_loop(0, 2 * len(ORDER), body, 0)

    per_link = 5 * half + 5 * quarter
    for link in links:
        link_copy(link, 0, tokens.at[pl.ds(0, per_link)]).wait_send()
    for i in range(4):
        ref = tokens.at[pl.ds(0, 8 * half)]
        pltpu.make_async_remote_copy(
            src_ref=ref, dst_ref=ref, send_sem=pair_send_sem.at[i], recv_sem=pair_sem.at[0, 0],
            device_id=device(chip, other), device_id_type=MESH).wait_send()


def drain(side, rows, q_in, k_in, v_in, last, wflat, q_out, k_out, v_out, tail, stage, main_sem, tail_sem):
    ins, outs = (q_in, k_in, v_in), (q_out, k_out, v_out)
    half = rows // 2
    heads = wflat.shape[1] // (3 * LANES)
    chip = lax.axis_index("tp") // CORES
    my_x, my_y = lax.rem(chip, side), chip // side

    def chip_at(dx, dy):
        return lax.rem(my_y + dy + side, side) * side + lax.rem(my_x + dx + side, side)

    first = len(ORDER) - TAIL
    for dx, dy in ORDER:
        has = (ORDER.index((dx, dy)) < first, ORDER.index((dy, dx)) < first)
        base = chip_at(dx, dy) * (CORES * rows)
        if has[0] and has[1]:
            parts = [(0, CORES * rows)]
        else:
            parts = [(c * rows + h * half, half) for c in range(CORES) for h in range(2) if has[h]]
        for off, n in parts:
            at = pl.ds(pl.multiple_of((base + off) * heads, half * heads), n * heads)
            for i in range(3):
                pltpu.make_async_copy(ins[i].at[at], outs[i].at[at], main_sem.at[i]).start()

    step_rows = 2 * half * heads

    def body(s, _):
        step, plane = first + s // 2, lax.rem(s, 2)
        dst = places(side, rows, heads, chip_at, step, plane)[1]
        src = [pl.multiple_of(((s // 2) * 2 + j) * (CORES * half) + plane * half, half) for j in range(2)]
        mine = [pl.multiple_of(s * step_rows + j * half * heads, half * heads) for j in range(2)]
        project(last, wflat, stage, src, half, tuple((tail.at[i], mine) for i in range(3)))
        for i in range(3):
            for j in range(2):
                pltpu.make_async_copy(tail.at[i, pl.ds(mine[j], half * heads)], outs[i].at[pl.ds(dst[j], half * heads)], tail_sem.at[i]).start()
        return 0

    lax.fori_loop(0, 2 * TAIL, body, 0)
    for i in range(3):
        n = first * CORES * step_rows
        pltpu.make_async_copy(ins[i].at[pl.ds(0, n)], outs[i].at[pl.ds(0, n)], main_sem.at[i]).wait()
        n = TAIL * CORES * step_rows
        pltpu.make_async_copy(tail.at[i], outs[i].at[pl.ds(0, n)], tail_sem.at[i]).wait()


def solution(mesh):
    size = mesh.shape["tp"]
    side = math.isqrt(size // CORES)
    assert side * side * CORES == size and side * side == len(ORDER)

    def local_step(x, gain, wq, wk, wv):
        rows, depth = x.shape
        heads = wq.shape[1]
        total = rows * size
        flat = [w.reshape(depth * heads, LANES) for w in (wq, wk, wv)]
        vmem_out = pltpu.VMEM((total * heads, LANES), jnp.bfloat16)
        outs = pl.pallas_call(
            functools.partial(gather_project, side),
            out_shape=(vmem_out,) * 3 + (pltpu.VMEM((TAIL * CORES * rows, depth), jnp.bfloat16), pltpu.VMEM((depth, 3 * heads * LANES), jnp.bfloat16)),
            in_specs=[pl.BlockSpec(memory_space=pl.ANY), pl.BlockSpec(memory_space=pltpu.VMEM)] + [pl.BlockSpec(memory_space=pl.ANY)] * 3,
            out_specs=[pl.BlockSpec(memory_space=pltpu.VMEM)] * 5,
            scratch_shapes=[
                pltpu.VMEM((rows, depth), jnp.bfloat16),
                pltpu.VMEM((total, depth), jnp.bfloat16),
                pltpu.VMEM((3, depth * heads, LANES), jnp.bfloat16),
                pltpu.VMEM((3, rows * heads, LANES), jnp.float32),
                pltpu.SemaphoreType.DMA((4,)),
                pltpu.SemaphoreType.DMA((4,)),
                pltpu.SemaphoreType.DMA((4,)),
                pltpu.SemaphoreType.DMA((4, 10)),
                pltpu.SemaphoreType.DMA((len(ORDER), 2)),
            ],
            compiler_params=pltpu.CompilerParams(collective_id=0, has_side_effects=True, vmem_limit_bytes=50 * 1024 * 1024 // 2),
            name="gather_project",
        )(x, gain.reshape(1, depth), *flat)
        out = jax.ShapeDtypeStruct((total * heads, LANES), jnp.bfloat16)
        outs = pl.pallas_call(
            functools.partial(drain, side, rows),
            out_shape=(out,) * 3,
            in_specs=[pl.BlockSpec(memory_space=pltpu.VMEM)] * 5,
            out_specs=[pl.BlockSpec(memory_space=pl.ANY)] * 3,
            scratch_shapes=[
                pltpu.VMEM((3, TAIL * CORES * rows * heads, LANES), jnp.bfloat16),
                pltpu.VMEM((3, rows * heads, LANES), jnp.float32),
                pltpu.SemaphoreType.DMA((3,)),
                pltpu.SemaphoreType.DMA((3,)),
            ],
            compiler_params=pltpu.CompilerParams(vmem_limit_bytes=48 * 1024 * 1024 // 2),
            name="drain",
        )(*outs)
        return tuple(o.reshape(total, heads, LANES) for o in outs)

    row_spec = P(("dp", "tp"), None)
    head_spec = P(None, "tp", None)
    out_spec = P("dp", "tp", None)
    return jax.shard_map(local_step, mesh=mesh, in_specs=(row_spec, P(None), head_spec, head_spec, head_spec),
                         out_specs=(out_spec, out_spec, out_spec), check_vma=False)
```

```python
import functools
import math

import jax
import jax.numpy as jnp
from jax import lax
from jax.experimental import pallas as pl
from jax.experimental.pallas import tpu as pltpu
from jax.sharding import PartitionSpec as P

MESH = pl.DeviceIdType.MESH
CORES = 2
LANES = 128

ORDER = ((0, 0), (-1, 0), (1, 0), (0, -1), (0, 1), (2, 0), (-1, -1), (-1, 1), (1, -1), (1, 1), (2, -1), (2, 1), (0, 2), (-1, 2), (1, 2), (2, 2))
XP, XM, YP, YM = range(4)


TAIL = 2
VMEM_LIMIT = 63438848 - 28311552 - TAIL * 1048576


def places(side, rows, heads, chip_at, step, plane):
    half = rows // 2
    dx, dy = jnp.int32(0), jnp.int32(0)
    for k, (ox, oy) in enumerate(ORDER):
        dx = jnp.where(step == k, ox, dx)
        dy = jnp.where(step == k, oy, dy)
    chips = (chip_at(dx, dy), chip_at(dy, dx))
    src = [pl.multiple_of(chips[i] * (CORES * rows) + i * (CORES * half) + plane * half, half) for i in range(2)]
    dst = [pl.multiple_of(((chips[i] * CORES + plane) * rows + i * half) * heads, half * heads) for i in range(2)]
    return src, dst


def project(tokens, wflat, stage, src, half, outs):
    lhs = jnp.concatenate([tokens[pl.ds(r, half), :] for r in src], axis=0)
    heads = wflat.shape[1] // (3 * LANES)
    cols = heads * LANES
    for i, (out, dst) in enumerate(outs):
        for b in range(cols // 256):
            acc = jnp.dot(lhs, wflat[:, pl.ds(i * cols + b * 256, 256)], preferred_element_type=jnp.float32)
            for h in range(2):
                stage[i, pl.ds(b * 2 + h, 2 * half, stride=heads), :] = acc[:, h * LANES:(h + 1) * LANES]
        for j in range(2):
            out[pl.ds(dst[j], half * heads), :] = stage[i, pl.ds(j * half * heads, half * heads), :].astype(jnp.bfloat16)


def gather_project(side, x_hbm, g_hbm, wq_hbm, wk_hbm, wv_hbm, q_ref, k_ref, v_ref, last, wflat, xbuf, g_ref, tokens, wraw, stage,
                   in_sem, send_sem, pair_send_sem, link_sem, pair_sem):
    rows, depth = xbuf.shape
    half, quarter = rows // 2, rows // 4
    heads = wraw.shape[1] // depth
    cols = heads * LANES
    me = lax.axis_index("tp")
    core = lax.rem(me, CORES)
    chip = me // CORES
    my_x, my_y = lax.rem(chip, side), chip // side

    def chip_at(dx, dy):
        return lax.rem(my_y + dy + side, side) * side + lax.rem(my_x + dx + side, side)

    def device(chip_index, core_index):
        return {"tp": chip_index * CORES + core_index}

    neighbour = (chip_at(1, 0), chip_at(-1, 0), chip_at(0, 1), chip_at(0, -1))
    other = 1 - core

    barrier = pltpu.get_barrier_semaphore()
    for chip_index in neighbour:
        pl.semaphore_signal(barrier, inc=1, device_id=device(chip_index, core), device_id_type=MESH)
    pl.semaphore_signal(barrier, inc=1, device_id=device(chip, other), device_id_type=MESH)

    halves_in = [pltpu.make_async_copy(x_hbm.at[pl.ds(h * half, half)], xbuf.at[pl.ds(h * half, half)], in_sem.at[h]) for h in range(2)]
    gain_in = pltpu.make_async_copy(g_hbm, g_ref, in_sem.at[2])
    weights_in = [pltpu.make_async_copy(w, wraw.at[i], in_sem.at[3 + i]) for i, w in enumerate((wq_hbm, wk_hbm, wv_hbm))]
    halves_in[0].start()
    gain_in.start()
    halves_in[1].start()

    def piece(dx, dy, is_q, part=None):
        start = chip_at(dx, dy) * (CORES * rows) + is_q * (CORES * half) + core * half
        if part is None:
            return tokens.at[pl.ds(pl.multiple_of(start, half), half)]
        return tokens.at[pl.ds(pl.multiple_of(start + part * quarter, quarter), quarter)]

    def last_piece(step, is_q, part=None):
        start = ((step - len(ORDER) + TAIL) * 2 + is_q) * (CORES * half) + core * half
        if part is None:
            return last.at[pl.ds(pl.multiple_of(start, half), half)]
        return last.at[pl.ds(pl.multiple_of(start + part * quarter, quarter), quarter)]

    def link_copy(link, seq, ref, dst=None):
        return pltpu.make_async_remote_copy(
            src_ref=ref, dst_ref=ref if dst is None else dst, send_sem=send_sem.at[link], recv_sem=link_sem.at[link, seq],
            device_id=device(neighbour[link], core), device_id_type=MESH)

    def pair_copy(step, is_q):
        dx, dy = ORDER[step]
        if step >= len(ORDER) - TAIL:
            ref = last_piece(step, is_q)
        else:
            ref = piece(dy, dx, 1) if is_q else piece(dx, dy, 0)
        return pltpu.make_async_remote_copy(
            src_ref=ref, dst_ref=ref, send_sem=pair_send_sem.at[step % 4], recv_sem=pair_sem.at[step, is_q],
            device_id=device(chip, other), device_id_type=MESH)

    def send(link, seq):
        is_y = link >= YP
        back = -1 if link in (XP, YP) else 1
        part = 0 if link in (XP, YP) else 1
        lateral = {1: 0, 3: -1, 4: 1, 5: 2, 6: 0, 7: -1, 8: 1, 9: 2}
        if seq == 0:
            off, second, sub = (0, 0), 0, None
        elif seq == 2:
            off, second, sub = (back, 0), 0, part
        elif seq in (1, 3, 4, 5):
            off, second, sub = (0, lateral[seq]), 1, None
        else:
            off, second, sub = (back, lateral[seq]), 1, part
        if is_y:
            off = (off[1], off[0])
        step = len(ORDER) - 10 + seq
        dst = last_piece(step, 1 - int(is_y), sub) if step >= len(ORDER) - TAIL else None
        link_copy(link, seq, piece(*off, second ^ int(is_y), sub), dst).start()

    def arrived(link, seq):
        n = quarter if seq in (2, 6, 7, 8, 9) else half
        link_copy(link, seq, tokens.at[pl.ds(0, n)]).wait_recv()

    links = (XP, XM, YP, YM)

    own = chip * (CORES * rows) + core * half
    norm_rows = 32
    gain_in.wait()
    for h in range(2):
        halves_in[h].wait()
        if h == 0:
            for copy in weights_in:
                copy.start()
        for r in range(0, half, norm_rows):
            xf = xbuf[pl.ds(h * half + r, norm_rows), :].astype(jnp.float32)
            mean_sq = jnp.mean(xf * xf, axis=-1, keepdims=True)
            n = (xf * lax.rsqrt(mean_sq + 1e-6) * g_ref[...]).astype(jnp.bfloat16)
            tokens[pl.ds(pl.multiple_of(own + h * (CORES * half) + r, norm_rows), norm_rows), :] = n
        if h == 0:
            pl.semaphore_wait(barrier, 5)
        for link in (links[:2] if h == 0 else links[2:]):
            send(link, 0)
        pair_copy(0, h).start()
    for link in links:
        send(link, 1)

    wrows = stage.shape[1] // heads
    for i in range(3):
        weights_in[i].wait()

        def relayout(j, _, i=i):
            src = pl.multiple_of(j * (wrows * heads), wrows * heads)
            dst = pl.multiple_of(j * wrows, wrows)
            stage[i] = wraw[i, pl.ds(src, wrows * heads), :].astype(jnp.float32)
            for h in range(heads):
                wflat[pl.ds(dst, wrows), pl.ds(i * cols + h * LANES, LANES)] = stage[i, pl.ds(h, wrows, stride=heads), :].astype(jnp.bfloat16)
            return 0

        lax.fori_loop(0, depth // wrows, relayout, 0)

    events = {
        1: ([(l, 0) for l in links], [(l, s) for s in (2, 3, 4) for l in links], (1, 2)),
        3: ([(l, 1) for l in links], [], (3, 4)),
        5: ([(l, 2) for l in links], [(l, s) for s in (5, 6) for l in links], (5,)),
        6: ([(l, 3) for l in links], [(l, 7) for l in links], (6, 7)),
        8: ([(l, 4) for l in links], [(l, 8) for l in links], (8, 9)),
        10: ([(l, 5) for l in links], [(l, 9) for l in links], (10, 11)),
        12: ([(l, 6) for l in links], [], (12,)),
        13: ([(l, 7) for l in links], [], (13,)),
        14: ([(l, 8) for l in links], [], (14,)),
        15: ([(l, 9) for l in links], [], (15,)),
    }

    def project_piece(step, plane):
        src, dst = places(side, rows, heads, chip_at, step, plane)
        project(tokens, wflat, stage, src, half, ((q_ref, dst), (k_ref, dst), (v_ref, dst)))

    def pair_arrived(step):
        for is_q in range(2):
            pltpu.make_async_remote_copy(
                src_ref=tokens.at[pl.ds(0, half)], dst_ref=tokens.at[pl.ds(0, half)], send_sem=pair_send_sem.at[0],
                recv_sem=pair_sem.at[step, is_q], device_id=device(chip, other), device_id_type=MESH).wait_recv()

    first = len(ORDER) - TAIL

    def body(s, _):
        step, sub = s // 2, lax.rem(s, 2)
        for at, (waits, sends, pairs) in events.items():
            @pl.when(s == 2 * at)
            def _(waits=waits, sends=sends, pairs=pairs):
                for w in waits:
                    arrived(*w)
                for x in sends:
                    send(*x)
                for p in pairs:
                    pair_copy(p, 0).start()
                    pair_copy(p, 1).start()

        @pl.when(jnp.logical_and(sub == 1, step > 0))
        def _():
            pair_arrived(step - 1)

        @pl.when(jnp.where(sub == 0, step < first, jnp.logical_and(step > 0, step <= first)))
        def _():
            project_piece(step - sub, core + sub * (1 - 2 * core))
        return 0

    lax.fori_loop(0, 2 * len(ORDER), body, 0)
    pair_arrived(len(ORDER) - 1)

    per_link = 5 * half + 5 * quarter
    for link in links:
        link_copy(link, 0, tokens.at[pl.ds(0, per_link)]).wait_send()
    for i in range(4):
        ref = tokens.at[pl.ds(0, 8 * half)]
        pltpu.make_async_remote_copy(
            src_ref=ref, dst_ref=ref, send_sem=pair_send_sem.at[i], recv_sem=pair_sem.at[0, 0],
            device_id=device(chip, other), device_id_type=MESH).wait_send()


def drain(side, rows, q_in, k_in, v_in, last, wflat, q_out, k_out, v_out, tail, stage, main_sem, tail_sem):
    ins, outs = (q_in, k_in, v_in), (q_out, k_out, v_out)
    half = rows // 2
    heads = wflat.shape[1] // (3 * LANES)
    chip = lax.axis_index("tp") // CORES
    my_x, my_y = lax.rem(chip, side), chip // side

    def chip_at(dx, dy):
        return lax.rem(my_y + dy + side, side) * side + lax.rem(my_x + dx + side, side)

    first = len(ORDER) - TAIL
    for dx, dy in ORDER:
        has = (ORDER.index((dx, dy)) < first, ORDER.index((dy, dx)) < first)
        base = chip_at(dx, dy) * (CORES * rows)
        if has[0] and has[1]:
            parts = [(0, CORES * rows)]
        else:
            parts = [(c * rows + h * half, half) for c in range(CORES) for h in range(2) if has[h]]
        for off, n in parts:
            at = pl.ds(pl.multiple_of((base + off) * heads, half * heads), n * heads)
            for i in range(3):
                pltpu.make_async_copy(ins[i].at[at], outs[i].at[at], main_sem.at[i]).start()

    step_rows = 2 * half * heads

    def body(s, _):
        step, plane = first + s // 2, lax.rem(s, 2)
        dst = places(side, rows, heads, chip_at, step, plane)[1]
        src = [pl.multiple_of(((s // 2) * 2 + j) * (CORES * half) + plane * half, half) for j in range(2)]
        mine = [pl.multiple_of(s * step_rows + j * half * heads, half * heads) for j in range(2)]
        project(last, wflat, stage, src, half, tuple((tail.at[i], mine) for i in range(3)))
        for i in range(3):
            for j in range(2):
                pltpu.make_async_copy(tail.at[i, pl.ds(mine[j], half * heads)], outs[i].at[pl.ds(dst[j], half * heads)], tail_sem.at[i]).start()
        return 0

    lax.fori_loop(0, 2 * TAIL, body, 0)
    for i in range(3):
        n = first * CORES * step_rows
        pltpu.make_async_copy(ins[i].at[pl.ds(0, n)], outs[i].at[pl.ds(0, n)], main_sem.at[i]).wait()
        n = TAIL * CORES * step_rows
        pltpu.make_async_copy(tail.at[i], outs[i].at[pl.ds(0, n)], tail_sem.at[i]).wait()


def solution(mesh):
    size = mesh.shape["tp"]
    side = math.isqrt(size // CORES)
    assert side * side * CORES == size and side * side == len(ORDER)

    def local_step(x, gain, wq, wk, wv):
        rows, depth = x.shape
        heads = wq.shape[1]
        total = rows * size
        flat = [w.reshape(depth * heads, LANES) for w in (wq, wk, wv)]
        vmem_out = pltpu.VMEM((total * heads, LANES), jnp.bfloat16)
        outs = pl.pallas_call(
            functools.partial(gather_project, side),
            out_shape=(vmem_out,) * 3 + (pltpu.VMEM((TAIL * CORES * rows, depth), jnp.bfloat16), pltpu.VMEM((depth, 3 * heads * LANES), jnp.bfloat16)),
            in_specs=[pl.BlockSpec(memory_space=pltpu.HBM)] * 5,
            out_specs=[pl.BlockSpec(memory_space=pltpu.VMEM)] * 5,
            scratch_shapes=[
                pltpu.VMEM((rows, depth), jnp.bfloat16),
                pltpu.VMEM((1, depth), jnp.float32),
                pltpu.VMEM((total, depth), jnp.bfloat16),
                pltpu.VMEM((3, depth * heads, LANES), jnp.bfloat16),
                pltpu.VMEM((3, rows * heads, LANES), jnp.float32),
                pltpu.SemaphoreType.DMA((6,)),
                pltpu.SemaphoreType.DMA((4,)),
                pltpu.SemaphoreType.DMA((4,)),
                pltpu.SemaphoreType.DMA((4, 10)),
                pltpu.SemaphoreType.DMA((len(ORDER), 2)),
            ],
            compiler_params=pltpu.CompilerParams(collective_id=0, has_side_effects=True, vmem_limit_bytes=50 * 1024 * 1024 // 2),
            name="gather_project",
        )(x, gain.reshape(1, depth), *flat)
        out = jax.ShapeDtypeStruct((total * heads, LANES), jnp.bfloat16)
        outs = pl.pallas_call(
            functools.partial(drain, side, rows),
            out_shape=(out,) * 3,
            in_specs=[pl.BlockSpec(memory_space=pltpu.VMEM)] * 5,
            out_specs=[pl.BlockSpec(memory_space=pl.ANY)] * 3,
            scratch_shapes=[
                pltpu.VMEM((3, TAIL * CORES * rows * heads, LANES), jnp.bfloat16),
                pltpu.VMEM((3, rows * heads, LANES), jnp.float32),
                pltpu.SemaphoreType.DMA((3,)),
                pltpu.SemaphoreType.DMA((3,)),
            ],
            compiler_params=pltpu.CompilerParams(vmem_limit_bytes=48 * 1024 * 1024 // 2),
            name="drain",
        )(*outs)
        return tuple(o.reshape(total, heads, LANES) for o in outs)

    row_spec = P(("dp", "tp"), None)
    head_spec = P(None, "tp", None)
    out_spec = P("dp", "tp", None)
    return jax.shard_map(local_step, mesh=mesh, in_specs=(row_spec, P(None), head_spec, head_spec, head_spec),
                         out_specs=(out_spec, out_spec, out_spec), check_vma=False)
```

```python
import functools
import math

import jax
import jax.numpy as jnp
from jax import lax
from jax.experimental import pallas as pl
from jax.experimental.pallas import tpu as pltpu
from jax.sharding import PartitionSpec as P

MESH = pl.DeviceIdType.MESH
CORES = 2
LANES = 128

ORDER = ((0, 0), (-1, 0), (1, 0), (0, -1), (0, 1), (2, 0), (-1, -1), (-1, 1), (1, -1), (1, 1), (2, -1), (2, 1), (0, 2), (-1, 2), (1, 2), (2, 2))
XP, XM, YP, YM = range(4)


TAIL = 2
VMEM_LIMIT = 63438848 - 28311552 - TAIL * 1048576


def places(side, rows, heads, chip_at, step, plane):
    half = rows // 2
    dx, dy = jnp.int32(0), jnp.int32(0)
    for k, (ox, oy) in enumerate(ORDER):
        dx = jnp.where(step == k, ox, dx)
        dy = jnp.where(step == k, oy, dy)
    chips = (chip_at(dx, dy), chip_at(dy, dx))
    src = [pl.multiple_of(chips[i] * (CORES * rows) + i * (CORES * half) + plane * half, half) for i in range(2)]
    dst = [pl.multiple_of(((chips[i] * CORES + plane) * rows + i * half) * heads, half * heads) for i in range(2)]
    return src, dst


def project(tokens, wflat, stage, src, half, outs):
    lhs = jnp.concatenate([tokens[pl.ds(r, half), :] for r in src], axis=0)
    heads = wflat.shape[1] // (3 * LANES)
    cols = heads * LANES
    for i, (out, dst) in enumerate(outs):
        for b in range(cols // 256):
            acc = jnp.dot(lhs, wflat[:, pl.ds(i * cols + b * 256, 256)], preferred_element_type=jnp.float32)
            for h in range(2):
                stage[i, pl.ds(b * 2 + h, 2 * half, stride=heads), :] = acc[:, h * LANES:(h + 1) * LANES]
        for j in range(2):
            out[pl.ds(dst[j], half * heads), :] = stage[i, pl.ds(j * half * heads, half * heads), :].astype(jnp.bfloat16)


def gather_project(side, x_hbm, g_hbm, wq_hbm, wk_hbm, wv_hbm, q_ref, k_ref, v_ref, last, wflat, xbuf, g_ref, tokens, wraw, stage,
                   in_sem, send_sem, link_sem, pair_sem):
    rows, depth = xbuf.shape
    half, quarter, eighth = rows // 2, rows // 4, rows // 8
    heads = wraw.shape[1] // depth
    cols = heads * LANES
    me = lax.axis_index("tp")
    core = lax.rem(me, CORES)
    chip = me // CORES
    my_x, my_y = lax.rem(chip, side), chip // side

    def chip_at(dx, dy):
        return lax.rem(my_y + dy + side, side) * side + lax.rem(my_x + dx + side, side)

    def device(chip_index, core_index):
        return {"tp": chip_index * CORES + core_index}

    neighbour = (chip_at(1, 0), chip_at(-1, 0), chip_at(0, 1), chip_at(0, -1))
    other = 1 - core

    barrier = pltpu.get_barrier_semaphore()
    for chip_index in neighbour:
        pl.semaphore_signal(barrier, inc=1, device_id=device(chip_index, core), device_id_type=MESH)
    pl.semaphore_signal(barrier, inc=1, device_id=device(chip, other), device_id_type=MESH)

    halves_in = [pltpu.make_async_copy(x_hbm.at[pl.ds(h * half, half)], xbuf.at[pl.ds(h * half, half)], in_sem.at[h]) for h in range(2)]
    gain_in = pltpu.make_async_copy(g_hbm, g_ref, in_sem.at[2])
    weights_in = [pltpu.make_async_copy(w, wraw.at[i], in_sem.at[3]) for i, w in enumerate((wq_hbm, wk_hbm, wv_hbm))]
    halves_in[0].start()
    gain_in.start()
    halves_in[1].start()

    def piece(dx, dy, is_q, part=None, sub=None):
        start = chip_at(dx, dy) * (CORES * rows) + is_q * (CORES * half) + core * half
        if part is None:
            return tokens.at[pl.ds(pl.multiple_of(start, half), half)]
        if sub is None:
            return tokens.at[pl.ds(pl.multiple_of(start + part * quarter, quarter), quarter)]
        return tokens.at[pl.ds(pl.multiple_of(start + part * quarter + sub * eighth, eighth), eighth)]

    def last_piece(step, is_q, part=None, sub=None):
        start = ((step - len(ORDER) + TAIL) * 2 + is_q) * (CORES * half) + core * half
        if part is None:
            return last.at[pl.ds(pl.multiple_of(start, half), half)]
        if sub is None:
            return last.at[pl.ds(pl.multiple_of(start + part * quarter, quarter), quarter)]
        return last.at[pl.ds(pl.multiple_of(start + part * quarter + sub * eighth, eighth), eighth)]

    def link_copy(link, seq, ref, dst=None):
        return pltpu.make_async_remote_copy(
            src_ref=ref, dst_ref=ref if dst is None else dst, send_sem=send_sem, recv_sem=link_sem.at[seq],
            device_id=device(neighbour[link], core), device_id_type=MESH)

    def to_pair(ref, sem):
        return pltpu.make_async_remote_copy(
            src_ref=ref, dst_ref=ref, send_sem=send_sem, recv_sem=pair_sem.at[sem],
            device_id=device(chip, other), device_id_type=MESH)

    def pair_copies(step):
        dx, dy = ORDER[step]
        if step >= len(ORDER) - TAIL:
            refs = [last_piece(step, 0), last_piece(step, 1)]
        else:
            refs = [piece(dx, dy, 0), piece(dy, dx, 1)]
        return [(ref, step) for ref in refs]

    def send(link, seq):
        is_y = link >= YP
        back = -1 if link in (XP, YP) else 1
        part = 0 if link in (XP, YP) else 1
        lateral = {1: 0, 3: -1, 4: 1, 5: 2, 6: 0, 7: -1, 8: 1, 9: 2, 10: 2}
        if seq == 0:
            off, second, sub = (0, 0), 0, None
        elif seq == 2:
            off, second, sub = (back, 0), 0, part
        elif seq in (1, 3, 4, 5):
            off, second, sub = (0, lateral[seq]), 1, None
        else:
            off, second, sub = (back, lateral[seq]), 1, part
        if is_y:
            off = (off[1], off[0])
        second = second ^ int(is_y)
        step = len(ORDER) - 10 + min(seq, 9)
        if seq >= 9:
            src = piece(*off, second, sub, seq - 9)
            dst = last_piece(step, second, sub, seq - 9)
        else:
            src = piece(*off, second, sub)
            dst = last_piece(step, second, sub) if step >= len(ORDER) - TAIL else None
        link_copy(link, seq, src, dst).start()

    def arrived(seq):
        n = 4 * (eighth if seq >= 9 else quarter if seq in (2, 6, 7, 8) else half)
        link_copy(XP, seq, tokens.at[pl.ds(0, n)]).wait_recv()

    links = (XP, XM, YP, YM)

    own = chip * (CORES * rows) + core * half
    norm_rows = 32
    gain_in.wait()
    for h in range(2):
        halves_in[h].wait()
        if h == 0:
            for copy in weights_in:
                copy.start()
        for r in range(0, half, norm_rows):
            xf = xbuf[pl.ds(h * half + r, norm_rows), :].astype(jnp.float32)
            mean_sq = jnp.mean(xf * xf, axis=-1, keepdims=True)
            n = (xf * lax.rsqrt(mean_sq + 1e-6) * g_ref[...]).astype(jnp.bfloat16)
            tokens[pl.ds(pl.multiple_of(own + h * (CORES * half) + r, norm_rows), norm_rows), :] = n
        if h == 0:
            pl.semaphore_wait(barrier, 5)
        for link in (links[:2] if h == 0 else links[2:]):
            send(link, 0)
        to_pair(*pair_copies(0)[h]).start()
    for link in links:
        send(link, 1)

    wrows = stage.shape[1] // heads
    pltpu.make_async_copy(wraw, wraw, in_sem.at[3]).wait()
    for i in range(3):

        def relayout(j, _, i=i):
            src = pl.multiple_of(j * (wrows * heads), wrows * heads)
            dst = pl.multiple_of(j * wrows, wrows)
            stage[i] = wraw[i, pl.ds(src, wrows * heads), :].astype(jnp.float32)
            for h in range(heads):
                wflat[pl.ds(dst, wrows), pl.ds(i * cols + h * LANES, LANES)] = stage[i, pl.ds(h, wrows, stride=heads), :].astype(jnp.bfloat16)
            return 0

        lax.fori_loop(0, depth // wrows, relayout, 0)

    events = {
        1: (0, (2, 3, 4), (1, 2)),
        3: (1, (), (3, 4)),
        5: (2, (5, 6), (5,)),
        6: (3, (7,), (6, 7)),
        8: (4, (8,), (8, 9)),
        10: (5, (9, 10), (10, 11)),
        12: (6, (), (12,)),
        13: (7, (), (13,)),
        14: (8, (), (14,)),
    }

    def project_piece(step, plane):
        src, dst = places(side, rows, heads, chip_at, step, plane)
        project(tokens, wflat, stage, src, half, ((q_ref, dst), (k_ref, dst), (v_ref, dst)))

    def pair_arrived(step):
        to_pair(tokens.at[pl.ds(0, 2 * half)], step).wait_recv()

    first = len(ORDER) - TAIL

    def body(s, _):
        step, sub = s // 2, lax.rem(s, 2)
        for at, (wait, sends, pairs) in events.items():
            @pl.when(s == 2 * at)
            def _(wait=wait, sends=sends, pairs=pairs):
                arrived(wait)
                for seq in sends:
                    for link in links:
                        send(link, seq)
                for p in pairs:
                    for copy in pair_copies(p):
                        to_pair(*copy).start()

        @pl.when(jnp.logical_and(sub == 1, step > 0))
        def _():
            pair_arrived(step - 1)

        @pl.when(jnp.where(sub == 0, step < first, jnp.logical_and(step > 0, step <= first)))
        def _():
            project_piece(step - sub, core + sub * (1 - 2 * core))
        return 0

    lax.fori_loop(0, 2 * len(ORDER) - 2, body, 0)

    end = len(ORDER) - 1
    for sub in range(2):
        arrived(9 + sub)
        for is_q in range(2):
            for part in range(2):
                to_pair(last_piece(end, is_q, part, sub), end + sub).start()
    pair_arrived(end - 1)
    for sub in range(2):
        to_pair(tokens.at[pl.ds(0, half)], end + sub).wait_recv()

    sent = 4 * (5 * half + 5 * quarter) + len(ORDER) * 2 * half
    to_pair(tokens.at[pl.ds(0, sent)], 0).wait_send()


def drain(side, rows, q_in, k_in, v_in, last, wflat, q_out, k_out, v_out, tail, stage, main_sem, tail_sem):
    ins, outs = (q_in, k_in, v_in), (q_out, k_out, v_out)
    half = rows // 2
    heads = wflat.shape[1] // (3 * LANES)
    chip = lax.axis_index("tp") // CORES
    my_x, my_y = lax.rem(chip, side), chip // side

    def chip_at(dx, dy):
        return lax.rem(my_y + dy + side, side) * side + lax.rem(my_x + dx + side, side)

    first = len(ORDER) - TAIL
    for dx, dy in ORDER:
        has = (ORDER.index((dx, dy)) < first, ORDER.index((dy, dx)) < first)
        base = chip_at(dx, dy) * (CORES * rows)
        if has[0] and has[1]:
            parts = [(0, CORES * rows)]
        else:
            parts = [(c * rows + h * half, half) for c in range(CORES) for h in range(2) if has[h]]
        for off, n in parts:
            at = pl.ds(pl.multiple_of((base + off) * heads, half * heads), n * heads)
            for i in range(3):
                pltpu.make_async_copy(ins[i].at[at], outs[i].at[at], main_sem.at[i]).start()

    step_rows = 2 * half * heads

    def body(s, _):
        step, plane = first + s // 2, lax.rem(s, 2)
        dst = places(side, rows, heads, chip_at, step, plane)[1]
        src = [pl.multiple_of(((s // 2) * 2 + j) * (CORES * half) + plane * half, half) for j in range(2)]
        mine = [pl.multiple_of(s * step_rows + j * half * heads, half * heads) for j in range(2)]
        project(last, wflat, stage, src, half, tuple((tail.at[i], mine) for i in range(3)))
        for i in range(3):
            for j in range(2):
                pltpu.make_async_copy(tail.at[i, pl.ds(mine[j], half * heads)], outs[i].at[pl.ds(dst[j], half * heads)], tail_sem.at[i]).start()
        return 0

    lax.fori_loop(0, 2 * TAIL, body, 0)
    for i in range(3):
        n = first * CORES * step_rows
        pltpu.make_async_copy(ins[i].at[pl.ds(0, n)], outs[i].at[pl.ds(0, n)], main_sem.at[i]).wait()
        n = TAIL * CORES * step_rows
        pltpu.make_async_copy(tail.at[i], outs[i].at[pl.ds(0, n)], tail_sem.at[i]).wait()


def solution(mesh):
    size = mesh.shape["tp"]
    side = math.isqrt(size // CORES)
    assert side * side * CORES == size and side * side == len(ORDER)

    def local_step(x, gain, wq, wk, wv):
        rows, depth = x.shape
        heads = wq.shape[1]
        total = rows * size
        flat = [w.reshape(depth * heads, LANES) for w in (wq, wk, wv)]
        vmem_out = pltpu.VMEM((total * heads, LANES), jnp.bfloat16)
        outs = pl.pallas_call(
            functools.partial(gather_project, side),
            out_shape=(vmem_out,) * 3 + (pltpu.VMEM((TAIL * CORES * rows, depth), jnp.bfloat16), pltpu.VMEM((depth, 3 * heads * LANES), jnp.bfloat16)),
            in_specs=[pl.BlockSpec(memory_space=pltpu.HBM)] * 5,
            out_specs=[pl.BlockSpec(memory_space=pltpu.VMEM)] * 5,
            scratch_shapes=[
                pltpu.VMEM((rows, depth), jnp.bfloat16),
                pltpu.VMEM((1, depth), jnp.float32),
                pltpu.VMEM((total, depth), jnp.bfloat16),
                pltpu.VMEM((3, depth * heads, LANES), jnp.bfloat16),
                pltpu.VMEM((3, rows * heads, LANES), jnp.float32),
                pltpu.SemaphoreType.DMA((4,)),
                pltpu.SemaphoreType.DMA,
                pltpu.SemaphoreType.DMA((11,)),
                pltpu.SemaphoreType.DMA((len(ORDER) + 1,)),
            ],
            compiler_params=pltpu.CompilerParams(collective_id=0, has_side_effects=True, vmem_limit_bytes=50 * 1024 * 1024 // 2),
            name="gather_project",
        )(x, gain.reshape(1, depth), *flat)
        out = jax.ShapeDtypeStruct((total * heads, LANES), jnp.bfloat16)
        outs = pl.pallas_call(
            functools.partial(drain, side, rows),
            out_shape=(out,) * 3,
            in_specs=[pl.BlockSpec(memory_space=pltpu.VMEM)] * 5,
            out_specs=[pl.BlockSpec(memory_space=pl.ANY)] * 3,
            scratch_shapes=[
                pltpu.VMEM((3, TAIL * CORES * rows * heads, LANES), jnp.bfloat16),
                pltpu.VMEM((3, rows * heads, LANES), jnp.float32),
                pltpu.SemaphoreType.DMA((3,)),
                pltpu.SemaphoreType.DMA((3,)),
            ],
            compiler_params=pltpu.CompilerParams(vmem_limit_bytes=48 * 1024 * 1024 // 2),
            name="drain",
        )(*outs)
        return tuple(o.reshape(total, heads, LANES) for o in outs)

    row_spec = P(("dp", "tp"), None)
    head_spec = P(None, "tp", None)
    out_spec = P("dp", "tp", None)
    return jax.shard_map(local_step, mesh=mesh, in_specs=(row_spec, P(None), head_spec, head_spec, head_spec),
                         out_specs=(out_spec, out_spec, out_spec), check_vma=False)
```

```python
import functools
import math

import jax
import jax.numpy as jnp
from jax import lax
from jax.experimental import pallas as pl
from jax.experimental.pallas import tpu as pltpu
from jax.sharding import PartitionSpec as P

MESH = pl.DeviceIdType.MESH
CORES = 2
LANES = 128

DIRECT = ((0, 0), (-1, 0), (1, 0), (-1, 0), (1, 0), (2, 0), (-1, -1), (1, -1), (-1, 1), (1, 1), (-1, 2), (1, 2), (2, 0), (2, -1), (2, 1), (2, 2))
MINE = (0, 1, 2, 5)
STEPS = len(DIRECT)
TAIL = 3
PARTS = 4


class Place:
    def __init__(self, side):
        self.side = side
        me = lax.axis_index("tp")
        self.core = lax.rem(me, CORES)
        self.other = 1 - self.core
        self.chip = me // CORES
        self.x, self.y = lax.rem(self.chip, side), self.chip // side

    def chip_at(self, axis, u, v):
        dx, dy = u + axis * (v - u), v + axis * (u - v)
        return lax.rem(self.y + dy + self.side, self.side) * self.side + lax.rem(self.x + dx + self.side, self.side)

    def block(self, axis, step):
        u, v, mine = jnp.int32(0), jnp.int32(0), jnp.int32(0)
        for k, (ku, kv) in enumerate(DIRECT):
            u = jnp.where(step == k, ku, u)
            v = jnp.where(step == k, kv, v)
            mine = jnp.where(step == k, int(k in MINE), mine)
        return self.chip_at(axis, u, v) * CORES + axis + (1 - mine) * (1 - 2 * axis)


def project(lhs, wflat, stage, outs):
    rows = lhs.shape[0]
    heads = wflat.shape[1] // (3 * LANES)
    cols = heads * LANES
    for i, (out, dst) in enumerate(outs):
        for b in range(cols // 256):
            acc = jnp.dot(lhs, wflat[:, pl.ds(i * cols + b * 256, 256)], preferred_element_type=jnp.float32)
            for h in range(2):
                stage[i, pl.ds(b * 2 + h, rows, stride=heads), :] = acc[:, h * LANES:(h + 1) * LANES]
        out[pl.ds(dst, rows * heads), :] = stage[i].astype(jnp.bfloat16)


def gather_project(side, x_hbm, g_hbm, wq_hbm, wk_hbm, wv_hbm, q_ref, k_ref, v_ref, last, wflat, xbuf, g_ref, tokens, wraw, stage,
                   in_sem, send_sem, link_sem, pair_sem):
    rows, depth = xbuf.shape
    half, part = rows // 2, rows // 2 // PARTS
    heads = wraw.shape[1] // depth
    cols = heads * LANES
    first = STEPS - TAIL
    here = Place(side)
    core, other = here.core, here.other

    halves_in = [pltpu.make_async_copy(x_hbm.at[pl.ds(h * half, half)], xbuf.at[pl.ds(h * half, half)], in_sem.at[h]) for h in range(2)]
    gain_in = pltpu.make_async_copy(g_hbm, g_ref, in_sem.at[2])
    halves_in[0].start()
    gain_in.start()
    halves_in[1].start()

    next_to = [here.chip_at(core, d, 0) * CORES + core for d in (1, -1)]
    partner = here.chip * CORES + other
    barrier = pltpu.get_barrier_semaphore()
    for dev in (*next_to, partner):
        pl.semaphore_signal(barrier, inc=1, device_id={"tp": dev}, device_id_type=MESH)

    def rows_of(u, v, mine, start=0, count=rows):
        dev = here.chip_at(core, u, v) * CORES + (core if mine else other)
        return tokens.at[pl.ds(pl.multiple_of(dev * rows + start, part), count)]

    def rows_of_last(step, start=0, count=rows):
        return last.at[pl.ds(pl.multiple_of(((step - first) * CORES + core) * rows + start, part), count)]

    def link_copy(way, sem, src, dst):
        return pltpu.make_async_remote_copy(
            src_ref=src, dst_ref=dst, send_sem=send_sem, recv_sem=link_sem.at[sem], device_id={"tp": next_to[way]}, device_id_type=MESH)

    def pair_copy(sem, ref):
        return pltpu.make_async_remote_copy(
            src_ref=ref, dst_ref=ref, send_sem=send_sem, recv_sem=pair_sem.at[sem], device_id={"tp": partner}, device_id_type=MESH)

    def send(way, seq, start=0, count=rows):
        back = (-1, 1)[way]
        if seq in (2, 6, 7, 8, 9):
            start, count = way * half + start, min(count, half)
        u, v, mine = {0: (0, 0, 1), 1: (0, 0, 0), 2: (back, 0, 1), 3: (0, -1, 0), 4: (0, 1, 0), 5: (0, 2, 0),
                      6: (back, 0, 0), 7: (back, -1, 0), 8: (back, 1, 0), 9: (back, 2, 0)}[seq]
        src = rows_of(u, v, mine, start, count)
        step = STEPS - 10 + seq
        dst = rows_of_last(step, start, count) if step >= first else src
        sem = seq if seq < 9 else 9 + (start - way * half) // part
        link_copy(way, sem, src, dst).start()

    def arrived(sem, count):
        ref = tokens.at[pl.ds(0, 2 * count)]
        link_copy(0, sem, ref, ref).wait_recv()

    def pair_arrived(sem, count=rows):
        pair_copy(sem, tokens.at[pl.ds(0, count)]).wait_recv()

    def hand_over(step):
        if step >= first:
            ref = rows_of_last(step)
        else:
            ref = rows_of(*DIRECT[step], step in MINE)
        pair_copy(step, ref).start()

    own = (here.chip * CORES + core) * rows
    norm_rows = 32
    gain_in.wait()
    for h in range(2):
        halves_in[h].wait()
        if h == 0:
            for i, w in enumerate((wq_hbm, wk_hbm, wv_hbm)):
                pltpu.make_async_copy(w, wraw.at[i], in_sem.at[3]).start()
        for r in range(h * half, (h + 1) * half, norm_rows):
            xf = xbuf[pl.ds(r, norm_rows), :].astype(jnp.float32)
            mean_sq = jnp.mean(xf * xf, axis=-1, keepdims=True)
            n = (xf * lax.rsqrt(mean_sq + 1e-6) * g_ref[...]).astype(jnp.bfloat16)
            tokens[pl.ds(pl.multiple_of(own + r, norm_rows), norm_rows), :] = n
        if h == 0:
            pl.semaphore_wait(barrier, 3)
        for way in range(2):
            send(way, 0, h * half, half)
    hand_over(0)

    wrows = stage.shape[1] // heads
    pltpu.make_async_copy(wraw, wraw, in_sem.at[3]).wait()
    for i in range(3):
        def relayout(j, _, i=i):
            src = pl.multiple_of(j * (wrows * heads), wrows * heads)
            dst = pl.multiple_of(j * wrows, wrows)
            stage[i] = wraw[i, pl.ds(src, wrows * heads), :].astype(jnp.float32)
            for h in range(heads):
                wflat[pl.ds(dst, wrows), pl.ds(i * cols + h * LANES, LANES)] = stage[i, pl.ds(h, wrows, stride=heads), :].astype(jnp.bfloat16)
            return 0

        lax.fori_loop(0, depth // wrows, relayout, 0)

    turns = {
        1: ((), (0,), (), (1,)),
        2: ((0,), (), (1, 2), (2,)),
        4: ((), (1, 2), (), (3, 4)),
        6: ((1,), (), (3, 4), ()),
        10: ((2,), (), (5,), ()),
        12: ((3,), (), (6, 7), ()),
        13: ((), (5,), (), (5, 6, 7)),
        16: ((4,), (), (8, 9), (8,)),
        20: ((5,), (), (10, 11), (9,)),
        24: ((6,), (), (12,), ()),
        26: ((7,), (), (13,), ()),
        28: ((8,), (), (14,), ()),
    }
    for step in range(first):
        if step not in (0, 1, 2, 5):
            turns[2 * step + 3] = ((), (step,), (), ())

    def body(s, _):
        step, sub = s // 2, lax.rem(s, 2)
        for at, (links, pairs, handed, sends) in turns.items():
            @pl.when(s == at)
            def _(links=links, pairs=pairs, handed=handed, sends=sends):
                for seq in links:
                    arrived(seq, half if seq in (2, 6, 7, 8) else rows)
                for p in pairs:
                    pair_arrived(p)
                for seq in sends:
                    for i in range(PARTS if seq == 9 else 1):
                        for way in range(2):
                            if seq == 9:
                                send(way, seq, i * part, part)
                            else:
                                send(way, seq)
                for p in handed:
                    hand_over(p)

        @pl.when(jnp.where(sub == 0, step < first, jnp.logical_and(step > 0, step <= first)))
        def _():
            row = here.block(core + sub * (1 - 2 * core), step - sub) * rows
            lhs = tokens[pl.ds(pl.multiple_of(row, rows), rows), :]
            dst = pl.multiple_of(row * heads, rows * heads)
            project(lhs, wflat, stage, ((q_ref, dst), (k_ref, dst), (v_ref, dst)))
        return 0

    lax.fori_loop(0, 2 * STEPS - 3, body, 0)

    end = STEPS - 1
    for i in range(PARTS):
        arrived(9 + i, part)
        for way in range(2):
            pair_copy(end + i, rows_of_last(end, way * half + i * part, part)).start()
    for step in range(first, end):
        pair_arrived(step)
    for i in range(PARTS):
        pair_arrived(end + i, 2 * part)

    sent = 2 * (5 * rows + 5 * half) + STEPS * rows
    pair_copy(0, tokens.at[pl.ds(0, sent)]).wait_send()


def drain(side, rows, q_in, k_in, v_in, last, wflat, q_out, k_out, v_out, tail, stage, main_sem, tail_sem):
    ins, outs = (q_in, k_in, v_in), (q_out, k_out, v_out)
    heads = wflat.shape[1] // (3 * LANES)
    first = STEPS - TAIL
    here = Place(side)

    late = [{(u, v) if axis == 0 else (v, u) for u, v in DIRECT[first:]} for axis in (1, 0)]
    for dx, dy in sorted(set(DIRECT) | {(v, u) for u, v in DIRECT}):
        base = here.chip_at(0, dx, dy) * (CORES * rows)
        keep = [c for c in range(CORES) if (dx, dy) not in late[c]]
        if not keep:
            continue
        at = pl.ds(pl.multiple_of((base + keep[0] * rows) * heads, rows * heads), len(keep) * rows * heads)
        for i in range(3):
            pltpu.make_async_copy(ins[i].at[at], outs[i].at[at], main_sem.at[i]).start()

    def body(s, _):
        src = pl.multiple_of(s * rows, rows)
        mine = pl.ds(pl.multiple_of(s * (rows * heads), rows * heads), rows * heads)
        dst = pl.ds(pl.multiple_of(here.block(lax.rem(s, 2), first + s // 2) * (rows * heads), rows * heads), rows * heads)
        project(last[pl.ds(src, rows), :], wflat, stage, tuple((tail.at[i], src * heads) for i in range(3)))
        for i in range(3):
            pltpu.make_async_copy(tail.at[i, mine], outs[i].at[dst], tail_sem.at[i]).start()
        return 0

    lax.fori_loop(0, CORES * TAIL, body, 0)
    for i in range(3):
        n = first * CORES * rows * heads
        pltpu.make_async_copy(ins[i].at[pl.ds(0, n)], outs[i].at[pl.ds(0, n)], main_sem.at[i]).wait()
        pltpu.make_async_copy(tail.at[i], outs[i].at[pl.ds(0, CORES * TAIL * rows * heads)], tail_sem.at[i]).wait()


def solution(mesh):
    size = mesh.shape["tp"]
    side = math.isqrt(size // CORES)
    assert side * side * CORES == size and side * side == STEPS

    def local_step(x, gain, wq, wk, wv):
        rows, depth = x.shape
        heads = wq.shape[1]
        total = rows * size
        flat = [w.reshape(depth * heads, LANES) for w in (wq, wk, wv)]
        vmem_out = pltpu.VMEM((total * heads, LANES), jnp.bfloat16)
        outs = pl.pallas_call(
            functools.partial(gather_project, side),
            out_shape=(vmem_out,) * 3 + (pltpu.VMEM((TAIL * CORES * rows, depth), jnp.bfloat16), pltpu.VMEM((depth, 3 * heads * LANES), jnp.bfloat16)),
            in_specs=[pl.BlockSpec(memory_space=pltpu.HBM)] * 5,
            out_specs=[pl.BlockSpec(memory_space=pltpu.VMEM)] * 5,
            scratch_shapes=[
                pltpu.VMEM((rows, depth), jnp.bfloat16),
                pltpu.VMEM((1, depth), jnp.float32),
                pltpu.VMEM((total, depth), jnp.bfloat16),
                pltpu.VMEM((3, depth * heads, LANES), jnp.bfloat16),
                pltpu.VMEM((3, rows * heads, LANES), jnp.float32),
                pltpu.SemaphoreType.DMA((4,)),
                pltpu.SemaphoreType.DMA,
                pltpu.SemaphoreType.DMA((9 + PARTS,)),
                pltpu.SemaphoreType.DMA((STEPS - 1 + PARTS,)),
            ],
            compiler_params=pltpu.CompilerParams(collective_id=0, has_side_effects=True, vmem_limit_bytes=98 * 1024 * 1024 // 4),
            name="gather_project",
        )(x, gain.reshape(1, depth), *flat)
        out = jax.ShapeDtypeStruct((total * heads, LANES), jnp.bfloat16)
        outs = pl.pallas_call(
            functools.partial(drain, side, rows),
            out_shape=(out,) * 3,
            in_specs=[pl.BlockSpec(memory_space=pltpu.VMEM)] * 5,
            out_specs=[pl.BlockSpec(memory_space=pl.ANY)] * 3,
            scratch_shapes=[
                pltpu.VMEM((3, TAIL * CORES * rows * heads, LANES), jnp.bfloat16),
                pltpu.VMEM((3, rows * heads, LANES), jnp.float32),
                pltpu.SemaphoreType.DMA((3,)),
                pltpu.SemaphoreType.DMA((3,)),
            ],
            compiler_params=pltpu.CompilerParams(vmem_limit_bytes=80 * 1024 * 1024 // 4),
            name="drain",
        )(*outs)
        return tuple(o.reshape(total, heads, LANES) for o in outs)

    row_spec = P(("dp", "tp"), None)
    head_spec = P(None, "tp", None)
    out_spec = P("dp", "tp", None)
    return jax.shard_map(local_step, mesh=mesh, in_specs=(row_spec, P(None), head_spec, head_spec, head_spec),
                         out_specs=(out_spec, out_spec, out_spec), check_vma=False)
```

```python
import functools
import math

import jax
import jax.numpy as jnp
from jax import lax
from jax.experimental import pallas as pl
from jax.experimental.pallas import tpu as pltpu
from jax.sharding import PartitionSpec as P

MESH = pl.DeviceIdType.MESH
CORES = 2
LANES = 128

DIRECT = ((0, 0), (-1, 0), (1, 0), (-1, 0), (1, 0), (2, 0), (-1, -1), (1, -1), (-1, 1), (1, 1), (-1, 2), (1, 2), (2, 0), (2, -1), (2, 1), (2, 2))
MINE = (0, 1, 2, 5)
STEPS = len(DIRECT)
PAIR_SEM = {0: 0, 1: 1, 2: 1, 3: 2, 4: 2, 5: 3, 6: 4, 7: 4, 8: 5, 9: 5, 10: 6, 11: 6, 12: 7, 13: 8, 14: 8, 15: 8}
TAIL = 3
PARTS = 8
X_PARTS = 8


class Place:
    def __init__(self, side):
        self.side = side
        me = lax.axis_index("tp")
        self.core = lax.rem(me, CORES)
        self.other = 1 - self.core
        self.chip = me // CORES
        self.x, self.y = lax.rem(self.chip, side), self.chip // side

    def chip_at(self, axis, u, v):
        dx, dy = u + axis * (v - u), v + axis * (u - v)
        return lax.rem(self.y + dy + self.side, self.side) * self.side + lax.rem(self.x + dx + self.side, self.side)

    def block(self, axis, step):
        u, v, mine = jnp.int32(0), jnp.int32(0), jnp.int32(0)
        for k, (ku, kv) in enumerate(DIRECT):
            u = jnp.where(step == k, ku, u)
            v = jnp.where(step == k, kv, v)
            mine = jnp.where(step == k, int(k in MINE), mine)
        return self.chip_at(axis, u, v) * CORES + axis + (1 - mine) * (1 - 2 * axis)


def project(lhs, wflat, stage, outs):
    rows = lhs.shape[0]
    heads = wflat.shape[1] // (3 * LANES)
    cols = heads * LANES
    for i, (out, dst) in enumerate(outs):
        for b in range(cols // 256):
            acc = jnp.dot(lhs, wflat[:, pl.ds(i * cols + b * 256, 256)], preferred_element_type=jnp.float32)
            for h in range(2):
                stage[i, pl.ds(b * 2 + h, rows, stride=heads), :] = acc[:, h * LANES:(h + 1) * LANES]
        out[pl.ds(dst, rows * heads), :] = stage[i].astype(jnp.bfloat16)


def gather_project(side, x_hbm, g_hbm, wq_hbm, wk_hbm, wv_hbm, q_ref, k_ref, v_ref, last, wflat, xbuf, g_ref, tokens, wraw, stage,
                   in_sem, send_sem, link_sem, pair_sem):
    rows, depth = xbuf.shape
    half, part = rows // 2, rows // 2 // PARTS
    heads = wraw.shape[1] // depth
    cols = heads * LANES
    first = STEPS - TAIL
    here = Place(side)
    core, other = here.core, here.other

    few = rows // X_PARTS
    x_in = [pltpu.make_async_copy(x_hbm.at[pl.ds(h * few, few)], xbuf.at[pl.ds(h * few, few)], in_sem.at[2 + h]) for h in range(X_PARTS)]
    gain_in = pltpu.make_async_copy(g_hbm, g_ref, in_sem.at[0])
    x_in[0].start()
    gain_in.start()
    for copy in x_in[1:]:
        copy.start()

    next_to = [here.chip_at(core, d, 0) * CORES + core for d in (1, -1)]
    partner = here.chip * CORES + other
    barrier = pltpu.get_barrier_semaphore()
    for dev in (*next_to, partner):
        pl.semaphore_signal(barrier, inc=1, device_id={"tp": dev}, device_id_type=MESH)

    def rows_of(u, v, mine, start=0, count=rows):
        dev = here.chip_at(core, u, v) * CORES + (core if mine else other)
        return tokens.at[pl.ds(pl.multiple_of(dev * rows + start, part), count)]

    def rows_of_last(step, start=0, count=rows):
        return last.at[pl.ds(pl.multiple_of(((step - first) * CORES + core) * rows + start, part), count)]

    def link_copy(way, sem, src, dst):
        return pltpu.make_async_remote_copy(
            src_ref=src, dst_ref=dst, send_sem=send_sem, recv_sem=link_sem.at[sem], device_id={"tp": next_to[way]}, device_id_type=MESH)

    def pair_copy(step, ref):
        return pltpu.make_async_remote_copy(
            src_ref=ref, dst_ref=ref, send_sem=send_sem, recv_sem=pair_sem.at[PAIR_SEM[step]], device_id={"tp": partner}, device_id_type=MESH)

    def send(way, seq, start=0, count=rows):
        back = (-1, 1)[way]
        if seq in (2, 6, 7, 8, 9):
            start, count = way * half + start, min(count, half)
        u, v, mine = {0: (0, 0, 1), 1: (0, 0, 0), 2: (back, 0, 1), 3: (0, -1, 0), 4: (0, 1, 0), 5: (0, 2, 0),
                      6: (back, 0, 0), 7: (back, -1, 0), 8: (back, 1, 0), 9: (back, 2, 0)}[seq]
        src = rows_of(u, v, mine, start, count)
        step = STEPS - 10 + seq
        dst = rows_of_last(step, start, count) if step >= first else src
        sem = seq if seq < 9 else 9 + (start - way * half) // part
        link_copy(way, sem, src, dst).start()

    def arrived(sem, count):
        ref = tokens.at[pl.ds(0, 2 * count)]
        link_copy(0, sem, ref, ref).wait_recv()

    def pair_arrived(step):
        together = sum(sem == PAIR_SEM[step] for sem in PAIR_SEM.values())
        pair_copy(step, tokens.at[pl.ds(0, together * rows)]).wait_recv()

    def hand_over(step):
        if step >= first:
            ref = rows_of_last(step)
        else:
            ref = rows_of(*DIRECT[step], step in MINE)
        pair_copy(step, ref).start()

    own = (here.chip * CORES + core) * rows
    norm_rows = 32
    gain_in.wait()
    for h in range(X_PARTS):
        x_in[h].wait()
        if h == X_PARTS - 1:
            for i, w in enumerate((wq_hbm, wk_hbm, wv_hbm)):
                pltpu.make_async_copy(w, wraw.at[i], in_sem.at[1]).start()
        for r in range(h * few, (h + 1) * few, norm_rows):
            xf = xbuf[pl.ds(r, norm_rows), :].astype(jnp.float32)
            mean_sq = jnp.mean(xf * xf, axis=-1, keepdims=True)
            n = (xf * lax.rsqrt(mean_sq + 1e-6) * g_ref[...]).astype(jnp.bfloat16)
            tokens[pl.ds(pl.multiple_of(own + r, norm_rows), norm_rows), :] = n
        if h == 0:
            pl.semaphore_wait(barrier, 3)
        for way in range(2):
            send(way, 0, h * few, few)
    hand_over(0)

    wrows = stage.shape[1] // heads
    pltpu.make_async_copy(wraw, wraw, in_sem.at[1]).wait()
    for i in range(3):
        def relayout(j, _, i=i):
            src = pl.multiple_of(j * (wrows * heads), wrows * heads)
            dst = pl.multiple_of(j * wrows, wrows)
            stage[i] = wraw[i, pl.ds(src, wrows * heads), :].astype(jnp.float32)
            for h in range(heads):
                wflat[pl.ds(dst, wrows), pl.ds(i * cols + h * LANES, LANES)] = stage[i, pl.ds(h, wrows, stride=heads), :].astype(jnp.bfloat16)
            return 0

        lax.fori_loop(0, depth // wrows, relayout, 0)

    turns = {
        1: ((), 0, (), (1,)),
        2: ((0,), None, (1, 2), (2,)),
        4: ((), 1, (), (3, 4)),
        6: ((1,), None, (3, 4), ()),
        10: ((2,), None, (5,), ()),
        12: ((3,), None, (6, 7), ()),
        13: ((), 5, (), (5, 6, 7)),
        16: ((4,), None, (8, 9), (8,)),
        20: ((5,), None, (10, 11), (9,)),
        24: ((6,), None, (12,), ()),
        26: ((7,), None, (13,), ()),
        28: ((8,), None, (14,), ()),
    }
    for step in (3, 6, 8, 10, 12):
        turns[2 * step + 3] = ((), step, (), ())

    def body(s, _):
        step, sub = s // 2, lax.rem(s, 2)
        for at, (links, pair, handed, sends) in turns.items():
            @pl.when(s == at)
            def _(links=links, pair=pair, handed=handed, sends=sends):
                for seq in links:
                    arrived(seq, half if seq in (2, 6, 7, 8) else rows)
                if pair is not None:
                    pair_arrived(pair)
                for seq in sends:
                    for i in range(PARTS if seq == 9 else 1):
                        for way in range(2):
                            if seq == 9:
                                send(way, seq, i * part, part)
                            else:
                                send(way, seq)
                for p in handed:
                    hand_over(p)

        @pl.when(jnp.where(sub == 0, step < first, jnp.logical_and(step > 0, step <= first)))
        def _():
            row = here.block(core + sub * (1 - 2 * core), step - sub) * rows
            lhs = tokens[pl.ds(pl.multiple_of(row, rows), rows), :]
            dst = pl.multiple_of(row * heads, rows * heads)
            project(lhs, wflat, stage, ((q_ref, dst), (k_ref, dst), (v_ref, dst)))
        return 0

    lax.fori_loop(0, 2 * STEPS - 3, body, 0)

    end = STEPS - 1
    for i in range(PARTS):
        arrived(9 + i, part)
        for way in range(2):
            pair_copy(end, rows_of_last(end, way * half + i * part, part)).start()
    pair_arrived(end)

    sent = 2 * (5 * rows + 5 * half) + STEPS * rows
    pair_copy(0, tokens.at[pl.ds(0, sent)]).wait_send()


def drain(side, rows, q_in, k_in, v_in, last, wflat, q_out, k_out, v_out, tail, stage, main_sem, tail_sem):
    ins, outs = (q_in, k_in, v_in), (q_out, k_out, v_out)
    heads = wflat.shape[1] // (3 * LANES)
    first = STEPS - TAIL
    here = Place(side)

    late = [{(u, v) if axis == 0 else (v, u) for u, v in DIRECT[first:]} for axis in (1, 0)]
    for dx, dy in sorted(set(DIRECT) | {(v, u) for u, v in DIRECT}):
        base = here.chip_at(0, dx, dy) * (CORES * rows)
        keep = [c for c in range(CORES) if (dx, dy) not in late[c]]
        if not keep:
            continue
        at = pl.ds(pl.multiple_of((base + keep[0] * rows) * heads, rows * heads), len(keep) * rows * heads)
        for i in range(3):
            pltpu.make_async_copy(ins[i].at[at], outs[i].at[at], main_sem.at[i]).start()

    def body(s, _):
        src = pl.multiple_of(s * rows, rows)
        mine = pl.ds(pl.multiple_of(s * (rows * heads), rows * heads), rows * heads)
        dst = pl.ds(pl.multiple_of(here.block(lax.rem(s, 2), first + s // 2) * (rows * heads), rows * heads), rows * heads)
        project(last[pl.ds(src, rows), :], wflat, stage, tuple((tail.at[i], src * heads) for i in range(3)))
        for i in range(3):
            pltpu.make_async_copy(tail.at[i, mine], outs[i].at[dst], tail_sem.at[i]).start()
        return 0

    lax.fori_loop(0, CORES * TAIL, body, 0)
    for i in range(3):
        n = first * CORES * rows * heads
        pltpu.make_async_copy(ins[i].at[pl.ds(0, n)], outs[i].at[pl.ds(0, n)], main_sem.at[i]).wait()
        pltpu.make_async_copy(tail.at[i], outs[i].at[pl.ds(0, CORES * TAIL * rows * heads)], tail_sem.at[i]).wait()


def solution(mesh):
    size = mesh.shape["tp"]
    side = math.isqrt(size // CORES)
    assert side * side * CORES == size and side * side == STEPS

    def local_step(x, gain, wq, wk, wv):
        rows, depth = x.shape
        heads = wq.shape[1]
        total = rows * size
        flat = [w.reshape(depth * heads, LANES) for w in (wq, wk, wv)]
        vmem_out = pltpu.VMEM((total * heads, LANES), jnp.bfloat16)
        outs = pl.pallas_call(
            functools.partial(gather_project, side),
            out_shape=(vmem_out,) * 3 + (pltpu.VMEM((TAIL * CORES * rows, depth), jnp.bfloat16), pltpu.VMEM((depth, 3 * heads * LANES), jnp.bfloat16)),
            in_specs=[pl.BlockSpec(memory_space=pltpu.HBM)] * 5,
            out_specs=[pl.BlockSpec(memory_space=pltpu.VMEM)] * 5,
            scratch_shapes=[
                pltpu.VMEM((rows, depth), jnp.bfloat16),
                pltpu.VMEM((1, depth), jnp.float32),
                pltpu.VMEM((total, depth), jnp.bfloat16),
                pltpu.VMEM((3, depth * heads, LANES), jnp.bfloat16),
                pltpu.VMEM((3, rows * heads, LANES), jnp.float32),
                pltpu.SemaphoreType.DMA((2 + X_PARTS,)),
                pltpu.SemaphoreType.DMA,
                pltpu.SemaphoreType.DMA((9 + PARTS,)),
                pltpu.SemaphoreType.DMA((max(PAIR_SEM.values()) + 1,)),
            ],
            compiler_params=pltpu.CompilerParams(collective_id=0, has_side_effects=True, vmem_limit_bytes=98 * 1024 * 1024 // 4),
            name="gather_project",
        )(x, gain.reshape(1, depth), *flat)
        out = jax.ShapeDtypeStruct((total * heads, LANES), jnp.bfloat16)
        outs = pl.pallas_call(
            functools.partial(drain, side, rows),
            out_shape=(out,) * 3,
            in_specs=[pl.BlockSpec(memory_space=pltpu.VMEM)] * 5,
            out_specs=[pl.BlockSpec(memory_space=pl.ANY)] * 3,
            scratch_shapes=[
                pltpu.VMEM((3, TAIL * CORES * rows * heads, LANES), jnp.bfloat16),
                pltpu.VMEM((3, rows * heads, LANES), jnp.float32),
                pltpu.SemaphoreType.DMA((3,)),
                pltpu.SemaphoreType.DMA((3,)),
            ],
            compiler_params=pltpu.CompilerParams(vmem_limit_bytes=80 * 1024 * 1024 // 4),
            name="drain",
        )(*outs)
        return tuple(o.reshape(total, heads, LANES) for o in outs)

    row_spec = P(("dp", "tp"), None)
    head_spec = P(None, "tp", None)
    out_spec = P("dp", "tp", None)
    return jax.shard_map(local_step, mesh=mesh, in_specs=(row_spec, P(None), head_spec, head_spec, head_spec),
                         out_specs=(out_spec, out_spec, out_spec), check_vma=False)
```

```python
import functools
import math

import jax
import jax.numpy as jnp
from jax import lax
from jax.experimental import pallas as pl
from jax.experimental.pallas import tpu as pltpu
from jax.sharding import PartitionSpec as P

MESH = pl.DeviceIdType.MESH
CORES = 2
LANES = 128

DIRECT = ((0, 0), (-1, 0), (1, 0), (-1, 0), (1, 0), (2, 0), (-1, -1), (1, -1), (-1, 1), (1, 1), (-1, 2), (1, 2), (2, 0), (2, -1), (2, 1), (2, 2))
MINE = (0, 1, 2, 5)
STEPS = len(DIRECT)
PAIR_SEM = {0: 0, 1: 1, 2: 1, 3: 2, 4: 2, 5: 3, 6: 4, 7: 4, 8: 5, 9: 5, 10: 6, 11: 6, 12: 7, 13: 8, 14: 8, 15: 8}
TAIL = 3
PARTS = 4
X_PARTS = 8


class Place:
    def __init__(self, side):
        self.side = side
        me = lax.axis_index("tp")
        self.core = lax.rem(me, CORES)
        self.other = 1 - self.core
        self.chip = me // CORES
        self.x, self.y = lax.rem(self.chip, side), self.chip // side

    def chip_at(self, axis, u, v):
        dx, dy = u + axis * (v - u), v + axis * (u - v)
        return lax.rem(self.y + dy + self.side, self.side) * self.side + lax.rem(self.x + dx + self.side, self.side)

    def block(self, axis, step):
        u, v, mine = jnp.int32(0), jnp.int32(0), jnp.int32(0)
        for k, (ku, kv) in enumerate(DIRECT):
            u = jnp.where(step == k, ku, u)
            v = jnp.where(step == k, kv, v)
            mine = jnp.where(step == k, int(k in MINE), mine)
        return self.chip_at(axis, u, v) * CORES + axis + (1 - mine) * (1 - 2 * axis)


def project(lhs, wflat, stage, outs):
    rows = lhs.shape[0]
    heads = wflat.shape[1] // (3 * LANES)
    cols = heads * LANES
    for i, (out, dst) in enumerate(outs):
        for b in range(cols // 256):
            acc = jnp.dot(lhs, wflat[:, pl.ds(i * cols + b * 256, 256)], preferred_element_type=jnp.float32)
            for h in range(2):
                stage[i, pl.ds(b * 2 + h, rows, stride=heads), :] = acc[:, h * LANES:(h + 1) * LANES]
        out[pl.ds(dst, rows * heads), :] = stage[i].astype(jnp.bfloat16)


def gather_project(side, x_hbm, g_hbm, wq_hbm, wk_hbm, wv_hbm, q_ref, k_ref, v_ref, last, wflat, xbuf, g_ref, tokens, wraw, stage,
                   in_sem, send_sem, link_sem, pair_sem, cross_sem):
    rows, depth = xbuf.shape
    half, part = rows // 2, rows // 2 // PARTS
    heads = wraw.shape[1] // depth
    cols = heads * LANES
    first = STEPS - TAIL
    here = Place(side)
    core, other = here.core, here.other

    few = rows // X_PARTS
    x_in = [pltpu.make_async_copy(x_hbm.at[pl.ds(h * few, few)], xbuf.at[pl.ds(h * few, few)], in_sem.at[2 + h]) for h in range(X_PARTS)]
    gain_in = pltpu.make_async_copy(g_hbm, g_ref, in_sem.at[0])
    x_in[0].start()
    gain_in.start()
    for copy in x_in[1:]:
        copy.start()

    next_to = [here.chip_at(core, d, 0) * CORES + core for d in (1, -1)]
    partner = here.chip * CORES + other
    barrier = pltpu.get_barrier_semaphore()
    for dev in (*next_to, partner):
        pl.semaphore_signal(barrier, inc=1, device_id={"tp": dev}, device_id_type=MESH)

    def rows_of(u, v, mine, start=0, count=rows):
        dev = here.chip_at(core, u, v) * CORES + (core if mine else other)
        return tokens.at[pl.ds(pl.multiple_of(dev * rows + start, part), count)]

    def rows_of_last(step, start=0, count=rows):
        return last.at[pl.ds(pl.multiple_of(((step - first) * CORES + core) * rows + start, part), count)]

    def link_copy(way, sem, src, dst):
        return pltpu.make_async_remote_copy(
            src_ref=src, dst_ref=dst, send_sem=send_sem, recv_sem=link_sem.at[sem], device_id={"tp": next_to[way]}, device_id_type=MESH)

    def cross_copy(way, ref):
        return pltpu.make_async_remote_copy(
            src_ref=ref[0], dst_ref=ref[1], send_sem=send_sem, recv_sem=cross_sem, device_id={"tp": next_to[way] + other - core}, device_id_type=MESH)

    def pair_copy(step, ref):
        return pltpu.make_async_remote_copy(
            src_ref=ref, dst_ref=ref, send_sem=send_sem, recv_sem=pair_sem.at[PAIR_SEM[step]], device_id={"tp": partner}, device_id_type=MESH)

    def send(way, seq, start=0, count=rows):
        back = (-1, 1)[way]
        if seq in (2, 6, 7, 8, 9):
            start, count = way * half + start, min(count, half)
        u, v, mine = {0: (0, 0, 1), 1: (0, 0, 0), 2: (back, 0, 1), 3: (0, -1, 0), 4: (0, 1, 0), 5: (0, 2, 0),
                      6: (back, 0, 0), 7: (back, -1, 0), 8: (back, 1, 0), 9: (back, 2, 0)}[seq]
        src = rows_of(u, v, mine, start, count)
        step = STEPS - 10 + seq
        dst = rows_of_last(step, start, count) if step >= first else src
        sem = seq if seq < 9 else 9 + (start - way * half) // part
        link_copy(way, sem, src, dst).start()
        if sem == 8 + PARTS:
            cross_copy(way, (src, dst)).start()

    def arrived(sem, count):
        ref = tokens.at[pl.ds(0, 2 * count)]
        link_copy(0, sem, ref, ref).wait_recv()

    def pair_arrived(step):
        together = sum(sem == PAIR_SEM[step] for sem in PAIR_SEM.values())
        crossed = 2 * part if step == STEPS - 1 else 0
        pair_copy(step, tokens.at[pl.ds(0, together * rows - crossed)]).wait_recv()

    def hand_over(step):
        if step >= first:
            ref = rows_of_last(step)
        else:
            ref = rows_of(*DIRECT[step], step in MINE)
        pair_copy(step, ref).start()

    own = (here.chip * CORES + core) * rows
    norm_rows = 32
    gain_in.wait()
    for h in range(X_PARTS):
        x_in[h].wait()
        if h == X_PARTS - 1:
            for i, w in enumerate((wq_hbm, wk_hbm, wv_hbm)):
                pltpu.make_async_copy(w, wraw.at[i], in_sem.at[1]).start()
        for r in range(h * few, (h + 1) * few, norm_rows):
            xf = xbuf[pl.ds(r, norm_rows), :].astype(jnp.float32)
            mean_sq = jnp.mean(xf * xf, axis=-1, keepdims=True)
            n = (xf * lax.rsqrt(mean_sq + 1e-6) * g_ref[...]).astype(jnp.bfloat16)
            tokens[pl.ds(pl.multiple_of(own + r, norm_rows), norm_rows), :] = n
        if h == 0:
            pl.semaphore_wait(barrier, 3)
        for way in range(2):
            send(way, 0, h * few, few)
    hand_over(0)

    wrows = stage.shape[1] // heads
    pltpu.make_async_copy(wraw, wraw, in_sem.at[1]).wait()
    for i in range(3):
        def relayout(j, _, i=i):
            src = pl.multiple_of(j * (wrows * heads), wrows * heads)
            dst = pl.multiple_of(j * wrows, wrows)
            stage[i] = wraw[i, pl.ds(src, wrows * heads), :].astype(jnp.float32)
            for h in range(heads):
                wflat[pl.ds(dst, wrows), pl.ds(i * cols + h * LANES, LANES)] = stage[i, pl.ds(h, wrows, stride=heads), :].astype(jnp.bfloat16)
            return 0

        lax.fori_loop(0, depth // wrows, relayout, 0)

    turns = {
        1: ((), 0, (), (1,)),
        2: ((0,), None, (1, 2), (2,)),
        4: ((), 1, (), (3, 4)),
        6: ((1,), None, (3, 4), ()),
        10: ((2,), None, (5,), ()),
        12: ((3,), None, (6, 7), ()),
        13: ((), 5, (), (5, 6, 7)),
        16: ((4,), None, (8, 9), (8,)),
        20: ((5,), None, (10, 11), (9,)),
        24: ((6,), None, (12,), ()),
        26: ((7,), None, (13,), ()),
        28: ((8,), None, (14,), ()),
    }
    for step in (3, 6, 8, 10, 12):
        turns[2 * step + 3] = ((), step, (), ())

    def body(s, _):
        step, sub = s // 2, lax.rem(s, 2)
        for at, (links, pair, handed, sends) in turns.items():
            @pl.when(s == at)
            def _(links=links, pair=pair, handed=handed, sends=sends):
                for seq in links:
                    arrived(seq, half if seq in (2, 6, 7, 8) else rows)
                if pair is not None:
                    pair_arrived(pair)
                for seq in sends:
                    for i in range(PARTS if seq == 9 else 1):
                        for way in range(2):
                            if seq == 9:
                                send(way, seq, i * part, part)
                            else:
                                send(way, seq)
                for p in handed:
                    hand_over(p)

        @pl.when(jnp.where(sub == 0, step < first, jnp.logical_and(step > 0, step <= first)))
        def _():
            row = here.block(core + sub * (1 - 2 * core), step - sub) * rows
            lhs = tokens[pl.ds(pl.multiple_of(row, rows), rows), :]
            dst = pl.multiple_of(row * heads, rows * heads)
            project(lhs, wflat, stage, ((q_ref, dst), (k_ref, dst), (v_ref, dst)))
        return 0

    lax.fori_loop(0, 2 * STEPS - 3, body, 0)

    end = STEPS - 1
    for i in range(PARTS):
        arrived(9 + i, part)
        for way in range(2 if i < PARTS - 1 else 0):
            pair_copy(end, rows_of_last(end, way * half + i * part, part)).start()
    pair_arrived(end)
    cross = tokens.at[pl.ds(0, 2 * part)]
    cross_copy(0, (cross, cross)).wait_recv()

    sent = 2 * (5 * rows + 5 * half) + STEPS * rows
    pair_copy(0, tokens.at[pl.ds(0, sent)]).wait_send()


def drain(side, rows, q_in, k_in, v_in, last, wflat, q_out, k_out, v_out, tail, stage, main_sem, tail_sem):
    ins, outs = (q_in, k_in, v_in), (q_out, k_out, v_out)
    heads = wflat.shape[1] // (3 * LANES)
    first = STEPS - TAIL
    here = Place(side)

    late = [{(u, v) if axis == 0 else (v, u) for u, v in DIRECT[first:]} for axis in (1, 0)]
    for dx, dy in sorted(set(DIRECT) | {(v, u) for u, v in DIRECT}):
        base = here.chip_at(0, dx, dy) * (CORES * rows)
        keep = [c for c in range(CORES) if (dx, dy) not in late[c]]
        if not keep:
            continue
        at = pl.ds(pl.multiple_of((base + keep[0] * rows) * heads, rows * heads), len(keep) * rows * heads)
        for i in range(3):
            pltpu.make_async_copy(ins[i].at[at], outs[i].at[at], main_sem.at[i]).start()

    def body(s, _):
        src = pl.multiple_of(s * rows, rows)
        mine = pl.ds(pl.multiple_of(s * (rows * heads), rows * heads), rows * heads)
        dst = pl.ds(pl.multiple_of(here.block(lax.rem(s, 2), first + s // 2) * (rows * heads), rows * heads), rows * heads)
        project(last[pl.ds(src, rows), :], wflat, stage, tuple((tail.at[i], src * heads) for i in range(3)))
        for i in range(3):
            pltpu.make_async_copy(tail.at[i, mine], outs[i].at[dst], tail_sem.at[i]).start()
        return 0

    lax.fori_loop(0, CORES * TAIL, body, 0)
    for i in range(3):
        n = first * CORES * rows * heads
        pltpu.make_async_copy(ins[i].at[pl.ds(0, n)], outs[i].at[pl.ds(0, n)], main_sem.at[i]).wait()
        pltpu.make_async_copy(tail.at[i], outs[i].at[pl.ds(0, CORES * TAIL * rows * heads)], tail_sem.at[i]).wait()


def solution(mesh):
    size = mesh.shape["tp"]
    side = math.isqrt(size // CORES)
    assert side * side * CORES == size and side * side == STEPS

    def local_step(x, gain, wq, wk, wv):
        rows, depth = x.shape
        heads = wq.shape[1]
        total = rows * size
        flat = [w.reshape(depth * heads, LANES) for w in (wq, wk, wv)]
        vmem_out = pltpu.VMEM((total * heads, LANES), jnp.bfloat16)
        outs = pl.pallas_call(
            functools.partial(gather_project, side),
            out_shape=(vmem_out,) * 3 + (pltpu.VMEM((TAIL * CORES * rows, depth), jnp.bfloat16), pltpu.VMEM((depth, 3 * heads * LANES), jnp.bfloat16)),
            in_specs=[pl.BlockSpec(memory_space=pltpu.HBM)] * 5,
            out_specs=[pl.BlockSpec(memory_space=pltpu.VMEM)] * 5,
            scratch_shapes=[
                pltpu.VMEM((rows, depth), jnp.bfloat16),
                pltpu.VMEM((1, depth), jnp.float32),
                pltpu.VMEM((total, depth), jnp.bfloat16),
                pltpu.VMEM((3, depth * heads, LANES), jnp.bfloat16),
                pltpu.VMEM((3, rows * heads, LANES), jnp.float32),
                pltpu.SemaphoreType.DMA((2 + X_PARTS,)),
                pltpu.SemaphoreType.DMA,
                pltpu.SemaphoreType.DMA((9 + PARTS,)),
                pltpu.SemaphoreType.DMA((max(PAIR_SEM.values()) + 1,)),
                pltpu.SemaphoreType.DMA,
            ],
            compiler_params=pltpu.CompilerParams(collective_id=0, has_side_effects=True, vmem_limit_bytes=98 * 1024 * 1024 // 4),
            name="gather_project",
        )(x, gain.reshape(1, depth), *flat)
        out = jax.ShapeDtypeStruct((total * heads, LANES), jnp.bfloat16)
        outs = pl.pallas_call(
            functools.partial(drain, side, rows),
            out_shape=(out,) * 3,
            in_specs=[pl.BlockSpec(memory_space=pltpu.VMEM)] * 5,
            out_specs=[pl.BlockSpec(memory_space=pl.ANY)] * 3,
            scratch_shapes=[
                pltpu.VMEM((3, TAIL * CORES * rows * heads, LANES), jnp.bfloat16),
                pltpu.VMEM((3, rows * heads, LANES), jnp.float32),
                pltpu.SemaphoreType.DMA((3,)),
                pltpu.SemaphoreType.DMA((3,)),
            ],
            compiler_params=pltpu.CompilerParams(vmem_limit_bytes=80 * 1024 * 1024 // 4),
            name="drain",
        )(*outs)
        return tuple(o.reshape(total, heads, LANES) for o in outs)

    row_spec = P(("dp", "tp"), None)
    head_spec = P(None, "tp", None)
    out_spec = P("dp", "tp", None)
    return jax.shard_map(local_step, mesh=mesh, in_specs=(row_spec, P(None), head_spec, head_spec, head_spec),
                         out_specs=(out_spec, out_spec, out_spec), check_vma=False)
```
